512 devices in a mesh: px: 16 (over y_lo, x, core), py: 32 (over y_hi, z).
Axes of the slice: x: 4, y: 8 (y_hi: 4, y_lo: 2; y = y_hi * 2 + y_lo), z: 8, core: 2. Of those that a mesh axis runs over, the one named last changes fastest.
Arguments:
- metric: bfloat16 [3, 640, 24, 4096], P(None, 'px', None, 'py'), may hold values from 0.25 to 24
- helmholtz: bfloat16 [640, 24, 4096], P('px', None, 'py'), may hold values from 1 to 30
- forcing: bfloat16 [640, 24, 4096], P('px', None, 'py'), may hold values from -6 to 6
- orientation: int32 [640, 4096], P('px', 'py'), may hold values 0 or 1
- start_x: float32 [640, 24, 4096], P('px', None, 'py'), may hold values from -6 to 6
- start_y: float32 [640, 24, 4096], P('px', None, 'py'), may hold values from -6 to 6
- start_z: float32 [640, 25, 4096], P('px', None, 'py'), may hold values from -6 to 6
Outputs:
- trace_x: float32 [640, 24, 4096], P('px', None, 'py')
- trace_y: float32 [640, 24, 4096], P('px', None, 'py')
- trace_z: float32 [640, 25, 4096], P('px', None, 'py')
- pressure: float32 [640, 24, 4096], P('px', None, 'py')
The draws below stay inside these ranges and needn't reach their ends.
All inputs are finite; a program needn't handle non-finite values. No bound on the sum of `orientation` on one device may be relied on, other than what follows from the above.
Results may differ from the reference program's by a relative error of at most 0.0003.
Values sent between devices are 32-bit elements; how exact they have to be, the bound alone decides.
A program may use at most 64 MiB of HBM per device.

```python
import math
import jax
import jax.numpy as jnp

L = 24
ITERS = 2
NX = 640
NY = 4096


def draw_metric(key, part):
    uniform_base = jax.random.uniform(key, (3, NX, L, NY), jnp.float32)
    across = (jnp.arange(NX, dtype=jnp.float32) / NX)[None, :, None, None]
    sideways = (jnp.arange(NY, dtype=jnp.float32) / NY)[None, None, None, :]
    tilt_factor = 3.0 ** across * 1.5 ** sideways
    spread = 0.5 * 8.0 ** uniform_base
    return (spread * tilt_factor).astype(jnp.bfloat16)


def set_ends(drawn, key, smallest, largest):
    extent = drawn.shape
    place = [jax.random.randint(jax.random.fold_in(key, axis), (), 0, extent[axis]) for axis in range(len(extent))]
    drawn = drawn.at[tuple(place)].set(smallest)
    longest = extent.index(max(extent))
    place[longest] = (place[longest] + 1) % extent[longest]
    return drawn.at[tuple(place)].set(largest)


def shard_levels(rng, extent, cuts, low, high):
    gain, own = 1.0, jax.random.fold_in(rng, 6)
    for dim, blocks in cuts:
        heights = jnp.exp(jax.random.uniform(jax.random.fold_in(own, dim), (blocks,), jnp.float32, low / len(cuts), high / len(cuts)))
        gain = gain * jnp.repeat(heights, extent[dim] // blocks).reshape([-1 if axis == dim else 1 for axis in range(len(extent))])
    return gain


def normal_values(key, shape, scale, most, shards=(), held_as=jnp.bfloat16):
    gain = shard_levels(key, shape, shards, -0.22, 0.18) if shards else 1.0
    array = jax.random.normal(key, shape, jnp.float32) * scale * gain
    return jnp.minimum(jnp.maximum(array, -most), most).astype(held_as)


def setup_inputs(seed: int = 0) -> dict:
    keys = jax.random.split(jax.random.key(seed), 8)
    return {
        "metric": draw_metric(jax.random.fold_in(keys[7], 71), 0),
        "helmholtz": jnp.clip(jnp.exp(math.log(30.0) - 3.4011974 * jax.random.uniform(keys[1], (NX, L, NY), jnp.float32) ** shard_levels(keys[1], (NX, L, NY), ((0, 16), (2, 32)), -0.2, 0.2)), 1.0, 30.0).astype(jnp.bfloat16),
        "forcing": normal_values(keys[2], (NX, L, NY), 1.0, 6.0, ((0, 16), (2, 32))),
        "orientation": set_ends((jax.random.randint(keys[3], (NX, NY), 0, 2) < 1).astype(jnp.int32), jax.random.fold_in(keys[3], 1), 0, 1),
        "start_x": normal_values(keys[4], (NX, L, NY), 1.0, 6.0, ((0, 16), (2, 32)), jnp.float32),
        "start_y": normal_values(keys[5], (NX, L, NY), 1.0, 6.0, ((0, 16), (2, 32)), jnp.float32),
        "start_z": normal_values(keys[6], (NX, L + 1, NY), 1.0, 6.0, ((0, 16), (2, 32)), jnp.float32),
    }


def coefficients(metric, helmholtz, orientation):
    metric_x = metric[0].astype(jnp.float32)
    metric_y = metric[1].astype(jnp.float32)
    metric_z = metric[2].astype(jnp.float32)
    turned = (orientation == 1)[:, None, :]
    inverse_x = 1.0 / jnp.where(turned, metric_y, metric_x)
    inverse_y = 1.0 / jnp.where(turned, metric_x, metric_y)
    inverse_z = 1.0 / metric_z
    denominator = helmholtz.astype(jnp.float32) + 2.0 * (3.0 * inverse_x + 3.0 * inverse_y + 3.0 * inverse_z)
    return (inverse_x, inverse_y, inverse_z, denominator)


def element(trace_west, trace_east, trace_south, trace_north, trace_bottom, trace_top, coeffs, source):
    inverse_x, inverse_y, inverse_z, denominator = coeffs
    weight_x = 3.0 * inverse_x
    weight_y = 3.0 * inverse_y
    weight_z = 3.0 * inverse_z
    gathered = weight_x * (trace_west + trace_east) + weight_y * (trace_south + trace_north) + weight_z * (trace_bottom + trace_top)
    pressure = (source + gathered) / denominator
    flux_west = inverse_x * (2.0 * trace_west + trace_east) - weight_x * pressure
    flux_east = inverse_x * (trace_west + 2.0 * trace_east) - weight_x * pressure
    flux_south = inverse_y * (2.0 * trace_south + trace_north) - weight_y * pressure
    flux_north = inverse_y * (trace_south + 2.0 * trace_north) - weight_y * pressure
    flux_bottom = inverse_z * (2.0 * trace_bottom + trace_top) - weight_z * pressure
    flux_top = inverse_z * (trace_bottom + 2.0 * trace_top) - weight_z * pressure
    return (flux_west, flux_east, flux_south, flux_north, flux_bottom, flux_top, pressure)


def stack_vertical(flux_bottom, flux_top):
    zero_layer = jnp.zeros_like(flux_bottom[:, :1])
    return jnp.concatenate([flux_bottom, zero_layer], 1) + jnp.concatenate([zero_layer, flux_top], 1)


def assemble(fields, coeffs, source):
    field_x, field_y, field_z = fields
    east_side = jnp.roll(field_x, -1, 0)
    north_side = jnp.roll(field_y, -1, 2)
    fluxes = element(field_x, east_side, field_y, north_side, field_z[:, :-1], field_z[:, 1:], coeffs, source)
    sum_x = fluxes[0] + jnp.roll(fluxes[1], 1, 0)
    sum_y = fluxes[2] + jnp.roll(fluxes[3], 1, 2)
    sum_z = stack_vertical(fluxes[4], fluxes[5])
    return (sum_x, sum_y, sum_z), fluxes[6]


def inner(first_vec, second_vec):
    return jnp.sum(first_vec[0] * second_vec[0]) + jnp.sum(first_vec[1] * second_vec[1]) + jnp.sum(first_vec[2] * second_vec[2])


def combine(first_vec, scale, second_vec):
    return tuple(member + scale * other for member, other in zip(first_vec, second_vec))


def reference(metric, helmholtz, forcing, orientation, start_x, start_y, start_z):
    coeffs = coefficients(metric, helmholtz, orientation)
    source = forcing.astype(jnp.float32)
    traces = (start_x, start_y, start_z)
    sums, unused = assemble(traces, coeffs, source)
    residual = tuple(-member for member in sums)
    direction = residual
    norm_now = inner(residual, residual)
    for iteration in range(ITERS):
        applied, unused = assemble(direction, coeffs, 0.0)
        step_size = norm_now / inner(direction, applied)
        traces = combine(traces, step_size, direction)
        residual = combine(residual, -step_size, applied)
        if iteration + 1 < ITERS:
            norm_next = inner(residual, residual)
            direction = combine(residual, norm_next / norm_now, direction)
            norm_now = norm_next
    unused, pressure = assemble(traces, coeffs, source)
    return (traces[0], traces[1], traces[2], pressure)
```

```python
import functools
import itertools

import jax
import jax.numpy as jnp
from jax import lax
from jax.experimental import pallas as pl
from jax.experimental.pallas import tpu as pltpu
from jax.sharding import PartitionSpec as P

MESH = pl.DeviceIdType.MESH
F32 = jnp.float32


def factors(px, py):
    if px == 16 and py == 32:
        return (2, 4, 2), (4, 8)
    return (1, px // 2, 2), (2, py // 2)


def peers(px, py, me_x, me_y, dims):
    (ny_lo, nx, nc), (ny_hi, nz) = factors(px, py)
    sizes = {"y_lo": ny_lo, "x": nx, "core": nc, "y_hi": ny_hi, "z": nz}
    here = {
        "core": lax.rem(me_x, nc),
        "x": lax.rem(me_x // nc, nx),
        "y_lo": me_x // (nc * nx),
        "z": lax.rem(me_y, nz),
        "y_hi": me_y // nz,
    }
    found = []
    for offset in itertools.product(*[range(sizes[d]) for d in dims]):
        if not any(offset):
            continue
        there = dict(here)
        for d, o in zip(dims, offset):
            there[d] = lax.rem(here[d] + o, sizes[d])
        found.append(
            {
                "px": (there["y_lo"] * nx + there["x"]) * nc + there["core"],
                "py": there["y_hi"] * nz + there["z"],
            }
        )
    return found


PHASES = (("core", "z"), ("x", "y_lo", "y_hi"))


def group_size(px, py, dims):
    (ny_lo, nx, nc), (ny_hi, nz) = factors(px, py)
    sizes = {"y_lo": ny_lo, "x": nx, "core": nc, "y_hi": ny_hi, "z": nz}
    total = 1
    for d in dims:
        total *= sizes[d]
    return total


def cell(w, e, s, n, b, t, ix, iy, iz, rd, g):
    sx, sy, sz = w + e, s + n, b + t
    total = 3.0 * (ix * sx + iy * sy + iz * sz)
    if g is not None:
        total = total + g
    p = total * rd
    p3 = 3.0 * p
    qx, qy, qz = sx - p3, sy - p3, sz - p3
    return (
        (ix * (qx + w), ix * (qx + e), iy * (qy + s), iy * (qy + n), iz * (qz + b), iz * (qz + t)),
        p,
    )


def halo_kernel(
    px, py,
    metric_h, helm_h, forc_h, orient_h, sx_h, sy_h, sz_h,
    x_ref, y_ref, z_ref, rx, ry, rz, wx, wy, wz, p0, p1, p2, coef,
    metric, helm, forc, orient, ix_s, iy_s, iz_s, rd_s,
    send_b, recv_b, row_b, *rest,
):
    slots = rest[: len(PHASES)]
    load_sem, send_sem, recv_sem, ar_send, ar_recv = rest[len(PHASES) :]
    n, levels, m = helm.shape
    me_x, me_y = lax.axis_index("px"), lax.axis_index("py")
    west = {"px": lax.rem(me_x + px - 1, px), "py": me_y}
    east = {"px": lax.rem(me_x + 1, px), "py": me_y}
    south = {"px": me_x, "py": lax.rem(me_y + py - 1, py)}
    north = {"px": me_x, "py": lax.rem(me_y + 1, py)}
    groups = [peers(px, py, me_x, me_y, dims) for dims in PHASES]

    barrier = pltpu.get_barrier_semaphore()
    greeted = [west, east, south, north] + [d for group in groups for d in group]
    for device in greeted:
        pl.semaphore_signal(barrier, inc=1, device_id=device, device_id_type=MESH)

    loads = [
        pltpu.make_async_copy(src, dst, load_sem.at[k])
        for k, (src, dst) in enumerate(
            [
                (sx_h, x_ref.at[pl.ds(0, n)]),
                (sy_h, y_ref),
                (metric_h, metric),
                (orient_h, orient),
                (helm_h, helm),
                (forc_h, forc),
                (sz_h, z_ref),
            ]
        )
    ]
    for load in loads:
        load.start()

    lane = lax.broadcasted_iota(jnp.int32, (levels, m), 1)
    level = lax.broadcasted_iota(jnp.int32, (levels, m), 0)
    zero = jnp.zeros((levels, m), F32)

    def exchange(k, device):
        return pltpu.make_async_remote_copy(
            src_ref=send_b.at[k],
            dst_ref=recv_b.at[k],
            send_sem=send_sem.at[k],
            recv_sem=recv_sem.at[k],
            device_id=device,
            device_id_type=MESH,
        )

    loads[0].wait()
    loads[1].wait()
    send_b[0] = x_ref[0]

    def pack(i, acc):
        return jnp.where(lane == i, pltpu.roll(y_ref[i], i, 1), acc)

    send_b[1] = lax.fori_loop(0, n, pack, zero, unroll=4)

    pl.semaphore_wait(barrier, len(greeted))
    first = [exchange(0, west), exchange(1, south)]
    for copy in first:
        copy.start()

    for load in loads[2:]:
        load.wait()

    def coefficient(i, carry):
        a = 1.0 / metric[0, i].astype(F32)
        b = 1.0 / metric[1, i].astype(F32)
        c = 1.0 / metric[2, i].astype(F32)
        turned = orient[pl.ds(i, 1), :] == 1
        ix_s[i] = jnp.where(turned, b, a)
        iy_s[i] = jnp.where(turned, a, b)
        iz_s[i] = c
        rd_s[i] = 1.0 / (helm[i].astype(F32) + 6.0 * (a + b + c))
        return carry

    lax.fori_loop(0, n, coefficient, 0, unroll=2)

    def northern(i, s, strip):
        rolled = pltpu.roll(s, m - 1, 1)
        return jnp.where(lane == m - 1, pltpu.roll(strip, m - 1 - i, 1), rolled)

    def to_lane0(i, strip):
        return jnp.where(lane == 0, pltpu.roll(strip, lax.rem(m - i, m), 1), 0.0)

    def vertical(i, ref):
        return ref[pl.ds(i, levels, stride=n), :], ref[pl.ds(i + n, levels, stride=n), :]

    def put_z(i, ref, fb, ft, sign):
        shifted = pltpu.roll(ft, 1, 0)
        body = fb + jnp.where(level == 0, 0.0, shifted)
        ref[pl.ds(i, levels, stride=n), :] = sign * body
        ref[pl.ds(i + levels * n, 1), :] = sign * shifted[0:1]

    def assemble(i, flux, fe_before, strips, outs, sign):
        fw, fe, fs, fn, fb, ft = flux
        out_x, out_y, out_z = outs
        out_x[i] = sign * (fw + fe_before)
        out_y[i] = sign * (fs + jnp.where(lane == 0, 0.0, pltpu.roll(fn, 1, 1)))
        put_z(i, out_z, fb, ft, sign)
        strip_s = jnp.where(lane == i, pltpu.roll(fs, i, 1), strips[0])
        strip_n = jnp.where(lane == i, pltpu.roll(fn, i + 1, 1), strips[1])
        return fe, (strip_s, strip_n)

    def send_partials(base, out_x, fe_last, strips, sign):
        send_b[base] = out_x[0]
        send_b[base + 1] = sign * fe_last
        send_b[base + 2] = sign * strips[0]
        send_b[base + 3] = sign * strips[1]
        copies = [exchange(base + k, d) for k, d in enumerate((west, east, south, north))]
        for copy in copies:
            copy.start()
        return copies

    def receive_partials(base, copies, out_x):
        for copy in copies:
            copy.wait_recv()
        out_x[0] = out_x[0] + recv_b[base + 1]
        out_x[n] = send_b[base + 1] + recv_b[base]
        return recv_b[base + 3], send_b[base + 3] + recv_b[base + 2]

    for copy in first:
        copy.wait_recv()
    x_ref[n] = recv_b[0]
    start_north = recv_b[1]

    def residual(i, carry):
        fe_before, strips = carry
        s = y_ref[i]
        b, t = vertical(i, z_ref)
        flux, p = cell(
            x_ref[i], x_ref[i + 1], s, northern(i, s, start_north), b, t,
            ix_s[i], iy_s[i], iz_s[i], rd_s[i], forc[i].astype(F32),
        )
        p0[i] = p
        return assemble(i, flux, fe_before, strips, (rx, ry, rz), -1.0)

    fe_last, strips = lax.fori_loop(0, n, residual, (zero, (zero, zero)))
    copies1 = send_partials(2, rx, fe_last, strips, -1.0)

    low, high = receive_partials(2, copies1, rx)

    def image(i, carry):
        fe_before, strips, rr = carry
        s = ry[i] + to_lane0(i, low)
        ry[i] = s
        b, t = vertical(i, rz)
        w = rx[i]
        flux, p = cell(
            w, rx[i + 1], s, northern(i, s, high), b, t,
            ix_s[i], iy_s[i], iz_s[i], rd_s[i], None,
        )
        p1[i] = p
        top = jnp.where(level == levels - 1, t, 0.0)
        rr = rr + (w * w + s * s + b * b + top * top)
        fe, strips = assemble(i, flux, fe_before, strips, (wx, wy, wz), 1.0)
        return fe, strips, rr

    fe_last, strips, rr = lax.fori_loop(0, n, image, (zero, (zero, zero), zero))
    copies2 = send_partials(6, wx, fe_last, strips, 1.0)

    low2, high2 = receive_partials(6, copies2, wx)

    def products(i, carry):
        rw, ww, waw = carry
        s = wy[i] + to_lane0(i, low2)
        wy[i] = s
        b, t = vertical(i, wz)
        rb, rt = vertical(i, rz)
        w, e = wx[i], wx[i + 1]
        north_side = northern(i, s, high2)
        flux, p = cell(
            w, e, s, north_side, b, t,
            ix_s[i], iy_s[i], iz_s[i], rd_s[i], None,
        )
        p2[i] = p
        top = jnp.where(level == levels - 1, t, 0.0)
        rw = rw + (w * rx[i] + s * ry[i] + b * rb + top * rt)
        ww = ww + (w * w + s * s + b * b + top * top)
        fw, fe, fs, fn, fb, ft = flux
        waw = waw + ((w * fw + e * fe) + (s * fs + north_side * fn) + (b * fb + t * ft))
        return rw, ww, waw

    rw, ww, waw = lax.fori_loop(0, n, products, (zero, zero, zero))

    lane_row = lax.broadcasted_iota(jnp.int32, (1, m), 1)
    row = jnp.zeros((1, m), F32)
    for k, part in enumerate((rr, rw, ww, waw)):
        whole = jnp.sum(jnp.sum(part, axis=0, keepdims=True), axis=1, keepdims=True)
        row = jnp.where(lane_row == k, whole, row)

    for k, (group, slot) in enumerate(zip(groups, slots)):
        row_b[k] = row
        for j, device in enumerate(group):
            pltpu.make_async_remote_copy(
                src_ref=row_b.at[pl.ds(k, 1)],
                dst_ref=slot.at[pl.ds(j, 1)],
                send_sem=ar_send.at[k],
                recv_sem=ar_recv.at[k],
                device_id=device,
                device_id_type=MESH,
            ).start()
        everything = pltpu.make_async_remote_copy(
            src_ref=slot, dst_ref=slot, send_sem=ar_send.at[k], recv_sem=ar_recv.at[k],
            device_id=group[0], device_id_type=MESH,
        )
        everything.wait_recv()
        row = row + jnp.sum(slot[...], axis=0)
        everything.wait_send()

    sums = [
        jnp.sum(jnp.where(lane_row == k, row, 0.0), axis=1, keepdims=True) for k in range(4)
    ]
    rr, rw, ww, waw = sums
    a0 = rr / rw
    grown = ww * a0 / rw
    b = grown - 1.0
    a1 = b * rr / (a0 * a0 * waw - grown * grown * rw)
    coef[0] = jnp.broadcast_to(a0 + a1 * grown, coef.shape[1:])
    coef[1] = jnp.broadcast_to(-a1 * a0, coef.shape[1:])
    for copy in first + copies1 + copies2:
        copy.wait_send()


def combine_kernel(
    x_ref, y_ref, z_ref, rx, ry, rz, wx, wy, wz, p0, p1, p2, coef,
    ox_h, oy_h, oz_h, op_h, ox, oy, oz, op, sem,
):
    n = ox.shape[0]
    chunks = 5
    rows = n // chunks
    step = n
    c1, c2 = coef[0, 0:1, :], coef[1, 0:1, :]
    copies = []
    for k in range(chunks):

        def body(i, carry):
            ox[i] = x_ref[i] + (c1 * rx[i] + c2 * wx[i])
            oy[i] = y_ref[i] + (c1 * ry[i] + c2 * wy[i])
            op[i] = p0[i] + (c1 * p1[i] + c2 * p2[i])
            return carry

        lax.fori_loop(k * rows, (k + 1) * rows, body, 0)
        tall = oz.shape[0] // chunks

        def body_z(i, carry):
            at = pl.ds(pl.multiple_of(i * step, step), step)
            oz[at, :] = z_ref[at, :] + (c1 * rz[at, :] + c2 * wz[at, :])
            return carry

        lax.fori_loop(k * (tall // step), (k + 1) * (tall // step), body_z, 0)
        span = pl.ds(k * rows, rows)
        span_z = pl.ds(k * tall, tall)
        for j, (src, dst, at) in enumerate(
            ((ox, ox_h, span), (oy, oy_h, span), (oz, oz_h, span_z), (op, op_h, span))
        ):
            copy = pltpu.make_async_copy(src.at[at], dst.at[at], sem.at[k, j])
            copy.start()
            copies.append(copy)
    for copy in copies:
        copy.wait()


def local(px, py, metric, helmholtz, forcing, orientation, start_x, start_y, start_z):
    n, levels, m = helmholtz.shape
    face = (n, levels, m)
    longer = (n + 1, levels, m)
    taller = ((levels + 1) * n, m)
    start_z = jnp.transpose(start_z, (1, 0, 2)).reshape(taller)
    arguments = [
        pltpu.with_memory_space_constraint(a, pltpu.HBM)
        for a in (metric, helmholtz, forcing, orientation, start_x, start_y, start_z)
    ]
    shapes = [longer, face, taller, longer, face, taller, longer, face, taller, face, face, face, (2, 8, m)]
    held = pl.pallas_call(
        functools.partial(halo_kernel, px, py),
        out_shape=[pltpu.VMEM(shape, F32) for shape in shapes],
        in_specs=[pl.BlockSpec(memory_space=pl.ANY)] * 7,
        out_specs=[pl.BlockSpec(memory_space=pltpu.VMEM)] * len(shapes),
        scratch_shapes=[
            pltpu.VMEM((3,) + face, metric.dtype),
            pltpu.VMEM(face, helmholtz.dtype),
            pltpu.VMEM(face, forcing.dtype),
            pltpu.VMEM((n, m), jnp.int32),
            pltpu.VMEM(face, F32),
            pltpu.VMEM(face, F32),
            pltpu.VMEM(face, F32),
            pltpu.VMEM(face, F32),
            pltpu.VMEM((10, levels, m), F32),
            pltpu.VMEM((10, levels, m), F32),
            pltpu.VMEM((len(PHASES), 1, m), F32),
        ]
        + [pltpu.VMEM((group_size(px, py, dims) - 1, 1, m), F32) for dims in PHASES]
        + [
            pltpu.SemaphoreType.DMA((7,)),
            pltpu.SemaphoreType.DMA((10,)),
            pltpu.SemaphoreType.DMA((10,)),
            pltpu.SemaphoreType.DMA((len(PHASES),)),
            pltpu.SemaphoreType.DMA((len(PHASES),)),
        ],
        compiler_params=pltpu.CompilerParams(
            collective_id=0, has_side_effects=True, vmem_limit_bytes=40 * 1024 * 1024
        ),
        name="halo",
    )(*arguments)
    outs = [face, face, taller, face]
    trace_x, trace_y, trace_z, pressure = pl.pallas_call(
        combine_kernel,
        out_shape=[jax.ShapeDtypeStruct(shape, F32) for shape in outs],
        in_specs=[pl.BlockSpec(memory_space=pltpu.VMEM)] * len(shapes),
        out_specs=[pl.BlockSpec(memory_space=pl.ANY)] * 4,
        scratch_shapes=[pltpu.VMEM(shape, F32) for shape in outs]
        + [pltpu.SemaphoreType.DMA((5, 4))],
        compiler_params=pltpu.CompilerParams(vmem_limit_bytes=20 * 1024 * 1024),
        name="combine",
    )(*held)
    trace_z = jnp.transpose(trace_z.reshape(levels + 1, n, m), (1, 0, 2))
    return trace_x, trace_y, trace_z, pressure


def solution(mesh):
    px, py = mesh.shape["px"], mesh.shape["py"]
    columns = P("px", None, "py")
    return jax.shard_map(
        functools.partial(local, px, py),
        mesh=mesh,
        in_specs=(P(None, "px", None, "py"), columns, columns, P("px", "py"), columns, columns, columns),
        out_specs=(columns,) * 4,
        check_vma=False,
    )
```

```python
import functools
import itertools

import jax
import jax.numpy as jnp
from jax import lax
from jax.experimental import pallas as pl
from jax.experimental.pallas import tpu as pltpu
from jax.sharding import PartitionSpec as P

MESH = pl.DeviceIdType.MESH
F32 = jnp.float32


def factors(px, py):
    if px == 16 and py == 32:
        return (2, 4, 2), (4, 8)
    return (1, px // 2, 2), (2, py // 2)


def peers(px, py, me_x, me_y, dims):
    (ny_lo, nx, nc), (ny_hi, nz) = factors(px, py)
    sizes = {"y_lo": ny_lo, "x": nx, "core": nc, "y_hi": ny_hi, "z": nz}
    here = {
        "core": lax.rem(me_x, nc),
        "x": lax.rem(me_x // nc, nx),
        "y_lo": me_x // (nc * nx),
        "z": lax.rem(me_y, nz),
        "y_hi": me_y // nz,
    }
    reach = {"core": 0, "x": 1, "y_lo": 1, "z": 1, "y_hi": 2}

    def far(offset):
        return sum(reach[d] * min(o, sizes[d] - o) for d, o in zip(dims, offset))

    found = []
    offsets = itertools.product(*[range(sizes[d]) for d in dims])
    for offset in sorted(offsets, key=far, reverse=True):
        if not any(offset):
            continue
        there = dict(here)
        for d, o in zip(dims, offset):
            there[d] = lax.rem(here[d] + o, sizes[d])
        found.append(
            {
                "px": (there["y_lo"] * nx + there["x"]) * nc + there["core"],
                "py": there["y_hi"] * nz + there["z"],
            }
        )
    return found


PHASES = (("core", "z"), ("x", "y_lo", "y_hi"))


def group_size(px, py, dims):
    (ny_lo, nx, nc), (ny_hi, nz) = factors(px, py)
    sizes = {"y_lo": ny_lo, "x": nx, "core": nc, "y_hi": ny_hi, "z": nz}
    total = 1
    for d in dims:
        total *= sizes[d]
    return total


def cell(w, e, s, n, b, t, ix, iy, iz, rd, g):
    sx, sy, sz = w + e, s + n, b + t
    total = 3.0 * (ix * sx + iy * sy + iz * sz)
    if g is not None:
        total = total + g
    p = total * rd
    p3 = 3.0 * p
    qx, qy, qz = sx - p3, sy - p3, sz - p3
    return (
        (ix * (qx + w), ix * (qx + e), iy * (qy + s), iy * (qy + n), iz * (qz + b), iz * (qz + t)),
        p,
    )


def halo_kernel(
    px, py,
    metric_h, helm_h, forc_h, orient_h, sx_h, sy_h, sz_h,
    x_ref, y_ref, z_ref, rx, ry, rz, wx, wy, wz, p0, p1, p2, coef,
    metric, helm, forc, orient, ix_s, iy_s, iz_s, rd_s,
    send_b, recv_b, row_b, *rest,
):
    slots = rest[: len(PHASES)]
    load_sem, send_sem, recv_sem, ar_send, ar_recv = rest[len(PHASES) :]
    n, levels, m = helm.shape
    me_x, me_y = lax.axis_index("px"), lax.axis_index("py")
    west = {"px": lax.rem(me_x + px - 1, px), "py": me_y}
    east = {"px": lax.rem(me_x + 1, px), "py": me_y}
    south = {"px": me_x, "py": lax.rem(me_y + py - 1, py)}
    north = {"px": me_x, "py": lax.rem(me_y + 1, py)}
    groups = [peers(px, py, me_x, me_y, dims) for dims in PHASES]

    barrier = pltpu.get_barrier_semaphore()
    greeted = [west, east, south, north] + [d for group in groups for d in group]
    for device in greeted:
        pl.semaphore_signal(barrier, inc=1, device_id=device, device_id_type=MESH)

    loads = [
        pltpu.make_async_copy(src, dst, load_sem.at[k])
        for k, (src, dst) in enumerate(
            [
                (sx_h, x_ref.at[pl.ds(0, n)]),
                (sy_h, y_ref),
                (metric_h, metric),
                (orient_h, orient),
                (helm_h, helm),
                (forc_h, forc),
                (sz_h, z_ref),
            ]
        )
    ]
    for load in loads:
        load.start()

    lane = lax.broadcasted_iota(jnp.int32, (levels, m), 1)
    level = lax.broadcasted_iota(jnp.int32, (levels, m), 0)
    zero = jnp.zeros((levels, m), F32)

    def exchange(k, device):
        return pltpu.make_async_remote_copy(
            src_ref=send_b.at[k],
            dst_ref=recv_b.at[k],
            send_sem=send_sem.at[k],
            recv_sem=recv_sem.at[k],
            device_id=device,
            device_id_type=MESH,
        )

    loads[0].wait()
    loads[1].wait()
    send_b[0] = x_ref[0]

    def pack(i, acc):
        return jnp.where(lane == i, pltpu.roll(y_ref[i], i, 1), acc)

    send_b[1] = lax.fori_loop(0, n, pack, zero, unroll=4)

    pl.semaphore_wait(barrier, len(greeted))
    first = [exchange(0, west), exchange(1, south)]
    for copy in first:
        copy.start()

    for load in loads[2:]:
        load.wait()

    def coefficient(i, carry):
        a = 1.0 / metric[0, i].astype(F32)
        b = 1.0 / metric[1, i].astype(F32)
        c = 1.0 / metric[2, i].astype(F32)
        turned = orient[pl.ds(i, 1), :] == 1
        ix_s[i] = jnp.where(turned, b, a)
        iy_s[i] = jnp.where(turned, a, b)
        iz_s[i] = c
        rd_s[i] = 1.0 / (helm[i].astype(F32) + 6.0 * (a + b + c))
        return carry

    lax.fori_loop(0, n, coefficient, 0, unroll=4)

    def northern(i, s, strip):
        rolled = pltpu.roll(s, m - 1, 1)
        return jnp.where(lane == m - 1, pltpu.roll(strip, m - 1 - i, 1), rolled)

    def to_lane0(i, strip):
        return jnp.where(lane == 0, pltpu.roll(strip, lax.rem(m - i, m), 1), 0.0)

    def vertical(i, ref):
        return ref[pl.ds(i, levels, stride=n), :], ref[pl.ds(i + n, levels, stride=n), :]

    def put_z(i, ref, fb, ft, sign):
        shifted = pltpu.roll(ft, 1, 0)
        body = fb + jnp.where(level == 0, 0.0, shifted)
        ref[pl.ds(i, levels, stride=n), :] = sign * body
        ref[pl.ds(i + levels * n, 1), :] = sign * shifted[0:1]

    def assemble(i, flux, fe_before, strips, outs, sign):
        fw, fe, fs, fn, fb, ft = flux
        out_x, out_y, out_z = outs
        out_x[i] = sign * (fw + fe_before)
        out_y[i] = sign * (fs + jnp.where(lane == 0, 0.0, pltpu.roll(fn, 1, 1)))
        put_z(i, out_z, fb, ft, sign)
        strip_s = jnp.where(lane == i, pltpu.roll(fs, i, 1), strips[0])
        strip_n = jnp.where(lane == i, pltpu.roll(fn, i + 1, 1), strips[1])
        return fe, (strip_s, strip_n)

    def send_partials(base, out_x, fe_last, strips, sign):
        send_b[base] = out_x[0]
        send_b[base + 1] = sign * fe_last
        send_b[base + 2] = sign * strips[0]
        send_b[base + 3] = sign * strips[1]
        copies = [exchange(base + k, d) for k, d in enumerate((west, east, south, north))]
        for copy in copies:
            copy.start()
        return copies

    def receive_partials(base, copies, out_x):
        for copy in copies:
            copy.wait_recv()
        out_x[0] = out_x[0] + recv_b[base + 1]
        out_x[n] = send_b[base + 1] + recv_b[base]
        return recv_b[base + 3], send_b[base + 3] + recv_b[base + 2]

    for copy in first:
        copy.wait_recv()
    x_ref[n] = recv_b[0]
    start_north = recv_b[1]

    def residual(i, carry):
        fe_before, strips = carry
        s = y_ref[i]
        b, t = vertical(i, z_ref)
        flux, p = cell(
            x_ref[i], x_ref[i + 1], s, northern(i, s, start_north), b, t,
            ix_s[i], iy_s[i], iz_s[i], rd_s[i], forc[i].astype(F32),
        )
        p0[i] = p
        return assemble(i, flux, fe_before, strips, (rx, ry, rz), -1.0)

    fe_last, strips = lax.fori_loop(0, n, residual, (zero, (zero, zero)), unroll=8)
    copies1 = send_partials(2, rx, fe_last, strips, -1.0)

    low, high = receive_partials(2, copies1, rx)

    def image(i, carry):
        fe_before, strips, rr = carry
        s = ry[i] + to_lane0(i, low)
        ry[i] = s
        b, t = vertical(i, rz)
        w = rx[i]
        flux, p = cell(
            w, rx[i + 1], s, northern(i, s, high), b, t,
            ix_s[i], iy_s[i], iz_s[i], rd_s[i], None,
        )
        p1[i] = p
        top = jnp.where(level == levels - 1, t, 0.0)
        rr = rr + (w * w + s * s + b * b + top * top)
        fe, strips = assemble(i, flux, fe_before, strips, (wx, wy, wz), 1.0)
        return fe, strips, rr

    fe_last, strips, rr = lax.fori_loop(0, n, image, (zero, (zero, zero), zero), unroll=8)
    copies2 = send_partials(6, wx, fe_last, strips, 1.0)

    low2, high2 = receive_partials(6, copies2, wx)

    def products(i, carry):
        rw, ww, waw = carry
        s = wy[i] + to_lane0(i, low2)
        wy[i] = s
        b, t = vertical(i, wz)
        rb, rt = vertical(i, rz)
        w, e = wx[i], wx[i + 1]
        north_side = northern(i, s, high2)
        flux, p = cell(
            w, e, s, north_side, b, t,
            ix_s[i], iy_s[i], iz_s[i], rd_s[i], None,
        )
        p2[i] = p
        top = jnp.where(level == levels - 1, t, 0.0)
        rw = rw + (w * rx[i] + s * ry[i] + b * rb + top * rt)
        ww = ww + (w * w + s * s + b * b + top * top)
        fw, fe, fs, fn, fb, ft = flux
        waw = waw + ((w * fw + e * fe) + (s * fs + north_side * fn) + (b * fb + t * ft))
        return rw, ww, waw

    rw, ww, waw = lax.fori_loop(0, n, products, (zero, zero, zero), unroll=8)

    lane_row = lax.broadcasted_iota(jnp.int32, (1, m), 1)
    row = jnp.zeros((1, m), F32)
    for k, part in enumerate((rr, rw, ww, waw)):
        whole = jnp.sum(jnp.sum(part, axis=0, keepdims=True), axis=1, keepdims=True)
        row = jnp.where(lane_row == k, whole, row)

    for k, (group, slot) in enumerate(zip(groups, slots)):
        row_b[k] = row
        for j, device in enumerate(group):
            pltpu.make_async_remote_copy(
                src_ref=row_b.at[pl.ds(k, 1)],
                dst_ref=slot.at[pl.ds(j, 1)],
                send_sem=ar_send.at[k],
                recv_sem=ar_recv.at[k],
                device_id=device,
                device_id_type=MESH,
            ).start()
        everything = pltpu.make_async_remote_copy(
            src_ref=slot, dst_ref=slot, send_sem=ar_send.at[k], recv_sem=ar_recv.at[k],
            device_id=group[0], device_id_type=MESH,
        )
        everything.wait_recv()
        row = row + jnp.sum(slot[...], axis=0)
        everything.wait_send()

    sums = [
        jnp.sum(jnp.where(lane_row == k, row, 0.0), axis=1, keepdims=True) for k in range(4)
    ]
    rr, rw, ww, waw = sums
    a0 = rr / rw
    grown = ww * a0 / rw
    b = grown - 1.0
    a1 = b * rr / (a0 * a0 * waw - grown * grown * rw)
    coef[0] = jnp.broadcast_to(a0 + a1 * grown, coef.shape[1:])
    coef[1] = jnp.broadcast_to(-a1 * a0, coef.shape[1:])
    for copy in first + copies1 + copies2:
        copy.wait_send()


def combine_kernel(
    x_ref, y_ref, z_ref, rx, ry, rz, wx, wy, wz, p0, p1, p2, coef,
    ox_h, oy_h, oz_h, op_h, ox, oy, oz, op, sem,
):
    n = ox.shape[0]
    chunks = 5
    rows = n // chunks
    step = n
    c1, c2 = coef[0, 0:1, :], coef[1, 0:1, :]
    copies = []
    for k in range(chunks):

        def body(i, carry):
            ox[i] = x_ref[i] + (c1 * rx[i] + c2 * wx[i])
            oy[i] = y_ref[i] + (c1 * ry[i] + c2 * wy[i])
            op[i] = p0[i] + (c1 * p1[i] + c2 * p2[i])
            return carry

        lax.fori_loop(k * rows, (k + 1) * rows, body, 0)
        tall = oz.shape[0] // chunks

        def body_z(i, carry):
            at = pl.ds(pl.multiple_of(i * step, step), step)
            oz[at, :] = z_ref[at, :] + (c1 * rz[at, :] + c2 * wz[at, :])
            return carry

        lax.fori_loop(k * (tall // step), (k + 1) * (tall // step), body_z, 0)
        span = pl.ds(k * rows, rows)
        span_z = pl.ds(k * tall, tall)
        for j, (src, dst, at) in enumerate(
            ((ox, ox_h, span), (oy, oy_h, span), (oz, oz_h, span_z), (op, op_h, span))
        ):
            copy = pltpu.make_async_copy(src.at[at], dst.at[at], sem.at[k, j])
            copy.start()
            copies.append(copy)
    for copy in copies:
        copy.wait()


def local(px, py, metric, helmholtz, forcing, orientation, start_x, start_y, start_z):
    n, levels, m = helmholtz.shape
    face = (n, levels, m)
    longer = (n + 1, levels, m)
    taller = ((levels + 1) * n, m)
    start_z = jnp.transpose(start_z, (1, 0, 2)).reshape(taller)
    arguments = [
        pltpu.with_memory_space_constraint(a, pltpu.HBM)
        for a in (metric, helmholtz, forcing, orientation, start_x, start_y, start_z)
    ]
    shapes = [longer, face, taller, longer, face, taller, longer, face, taller, face, face, face, (2, 8, m)]
    held = pl.pallas_call(
        functools.partial(halo_kernel, px, py),
        out_shape=[pltpu.VMEM(shape, F32) for shape in shapes],
        in_specs=[pl.BlockSpec(memory_space=pl.ANY)] * 7,
        out_specs=[pl.BlockSpec(memory_space=pltpu.VMEM)] * len(shapes),
        scratch_shapes=[
            pltpu.VMEM((3,) + face, metric.dtype),
            pltpu.VMEM(face, helmholtz.dtype),
            pltpu.VMEM(face, forcing.dtype),
            pltpu.VMEM((n, m), jnp.int32),
            pltpu.VMEM(face, F32),
            pltpu.VMEM(face, F32),
            pltpu.VMEM(face, F32),
            pltpu.VMEM(face, F32),
            pltpu.VMEM((10, levels, m), F32),
            pltpu.VMEM((10, levels, m), F32),
            pltpu.VMEM((len(PHASES), 1, m), F32),
        ]
        + [pltpu.VMEM((group_size(px, py, dims) - 1, 1, m), F32) for dims in PHASES]
        + [
            pltpu.SemaphoreType.DMA((7,)),
            pltpu.SemaphoreType.DMA((10,)),
            pltpu.SemaphoreType.DMA((10,)),
            pltpu.SemaphoreType.DMA((len(PHASES),)),
            pltpu.SemaphoreType.DMA((len(PHASES),)),
        ],
        compiler_params=pltpu.CompilerParams(
            collective_id=0, has_side_effects=True, vmem_limit_bytes=40 * 1024 * 1024
        ),
        name="halo",
    )(*arguments)
    outs = [face, face, taller, face]
    trace_x, trace_y, trace_z, pressure = pl.pallas_call(
        combine_kernel,
        out_shape=[jax.ShapeDtypeStruct(shape, F32) for shape in outs],
        in_specs=[pl.BlockSpec(memory_space=pltpu.VMEM)] * len(shapes),
        out_specs=[pl.BlockSpec(memory_space=pl.ANY)] * 4,
        scratch_shapes=[pltpu.VMEM(shape, F32) for shape in outs]
        + [pltpu.SemaphoreType.DMA((5, 4))],
        compiler_params=pltpu.CompilerParams(vmem_limit_bytes=20 * 1024 * 1024),
        name="combine",
    )(*held)
    trace_z = jnp.transpose(trace_z.reshape(levels + 1, n, m), (1, 0, 2))
    return trace_x, trace_y, trace_z, pressure


def solution(mesh):
    px, py = mesh.shape["px"], mesh.shape["py"]
    columns = P("px", None, "py")
    return jax.shard_map(
        functools.partial(local, px, py),
        mesh=mesh,
        in_specs=(P(None, "px", None, "py"), columns, columns, P("px", "py"), columns, columns, columns),
        out_specs=(columns,) * 4,
        check_vma=False,
    )
```

```python
import functools
import itertools

import jax
import jax.numpy as jnp
from jax import lax
from jax.experimental import pallas as pl
from jax.experimental.pallas import tpu as pltpu
from jax.sharding import PartitionSpec as P

MESH = pl.DeviceIdType.MESH
F32 = jnp.float32


def factors(px, py):
    if px == 16 and py == 32:
        return (2, 4, 2), (4, 8)
    return (1, px // 2, 2), (2, py // 2)


def peers(px, py, me_x, me_y, dims):
    (ny_lo, nx, nc), (ny_hi, nz) = factors(px, py)
    sizes = {"y_lo": ny_lo, "x": nx, "core": nc, "y_hi": ny_hi, "z": nz}
    here = {
        "core": lax.rem(me_x, nc),
        "x": lax.rem(me_x // nc, nx),
        "y_lo": me_x // (nc * nx),
        "z": lax.rem(me_y, nz),
        "y_hi": me_y // nz,
    }
    reach = {"core": 0, "x": 1, "y_lo": 1, "z": 1, "y_hi": 2}

    def far(offset):
        return sum(reach[d] * min(o, sizes[d] - o) for d, o in zip(dims, offset))

    found = []
    offsets = itertools.product(*[range(sizes[d]) for d in dims])
    for offset in sorted(offsets, key=far, reverse=True):
        if not any(offset):
            continue
        there = dict(here)
        for d, o in zip(dims, offset):
            there[d] = lax.rem(here[d] + o, sizes[d])
        found.append(
            {
                "px": (there["y_lo"] * nx + there["x"]) * nc + there["core"],
                "py": there["y_hi"] * nz + there["z"],
            }
        )
    return found


PHASES = (("core", "z"), ("x", "y_lo", "y_hi"))


def group_size(px, py, dims):
    (ny_lo, nx, nc), (ny_hi, nz) = factors(px, py)
    sizes = {"y_lo": ny_lo, "x": nx, "core": nc, "y_hi": ny_hi, "z": nz}
    total = 1
    for d in dims:
        total *= sizes[d]
    return total


def cell(w, e, s, n, b, t, ix, iy, iz, rd, g):
    sx, sy, sz = w + e, s + n, b + t
    total = 3.0 * (ix * sx + iy * sy + iz * sz)
    if g is not None:
        total = total + g
    p = total * rd
    p3 = 3.0 * p
    qx, qy, qz = sx - p3, sy - p3, sz - p3
    return (
        (ix * (qx + w), ix * (qx + e), iy * (qy + s), iy * (qy + n), iz * (qz + b), iz * (qz + t)),
        p,
    )


def halo_kernel(
    px, py,
    metric_h, helm_h, forc_h, orient_h, sx_h, sy_h, sz_h,
    x_ref, y_ref, z_ref, rx, ry, rz, wx, wy, wz, p0, p1, p2, coef,
    metric, helm, forc, orient, ix_s, iy_s, iz_s, rd_s,
    z_x, rz_x, wz_x, tb, send_b, recv_b, row_b, *rest,
):
    slots = rest[: len(PHASES)]
    load_sem, send_sem, recv_sem, ar_send, ar_recv = rest[len(PHASES) :]
    n, levels, m = helm.shape
    me_x, me_y = lax.axis_index("px"), lax.axis_index("py")
    west = {"px": lax.rem(me_x + px - 1, px), "py": me_y}
    east = {"px": lax.rem(me_x + 1, px), "py": me_y}
    south = {"px": me_x, "py": lax.rem(me_y + py - 1, py)}
    north = {"px": me_x, "py": lax.rem(me_y + 1, py)}
    groups = [peers(px, py, me_x, me_y, dims) for dims in PHASES]

    loads = [
        pltpu.make_async_copy(src, dst, load_sem.at[k])
        for k, (src, dst) in enumerate(
            [
                (sy_h, y_ref),
                (sx_h, x_ref.at[pl.ds(0, n)]),
                (metric_h, metric),
                (orient_h, orient),
                (helm_h, helm),
                (forc_h, forc),
                (sz_h, z_ref),
            ]
        )
    ]
    for load in loads:
        load.start()

    barrier = pltpu.get_barrier_semaphore()
    greeted = [west, east, south, north] + [d for group in groups for d in group]
    for device in greeted:
        pl.semaphore_signal(barrier, inc=1, device_id=device, device_id_type=MESH)

    lane = lax.broadcasted_iota(jnp.int32, (levels, m), 1)
    level = lax.broadcasted_iota(jnp.int32, (levels, m), 0)
    pair = jnp.right_shift(lane, 1)
    odd = jnp.bitwise_and(lane, 1) == 1
    zero = jnp.zeros((levels, m), F32)

    def into_strip(i, value, strip):
        return jnp.where(pair == i, pltpu.roll(value, 2 * i + 1, 1), strip)

    def lane1_into_strip(i, value, strip):
        return jnp.where(lane == 2 * i + 1, pltpu.roll(value, 2 * i, 1), strip)

    def exchange(source, slot, device):
        return pltpu.make_async_remote_copy(
            src_ref=send_b.at[source],
            dst_ref=recv_b.at[slot],
            send_sem=send_sem.at[slot],
            recv_sem=recv_sem.at[slot],
            device_id=device,
            device_id_type=MESH,
        )

    loads[0].wait()
    loads[1].wait()
    send_b[0] = x_ref[0]
    start_y = lax.fori_loop(0, n, lambda i, acc: into_strip(i, y_ref[i], acc), zero, unroll=20)
    send_b[1] = start_y

    pl.semaphore_wait(barrier, len(greeted))
    first = [exchange(0, 0, west), exchange(1, 1, south)]
    for copy in first:
        copy.start()

    for load in loads[2:]:
        load.wait()

    def coefficient(i, strips):
        a = 1.0 / metric[0, i].astype(F32)
        b = 1.0 / metric[1, i].astype(F32)
        c = 1.0 / metric[2, i].astype(F32)
        turned = orient[pl.ds(i, 1), :] == 1
        values = (
            jnp.where(turned, b, a),
            jnp.where(turned, a, b),
            c,
            1.0 / (helm[i].astype(F32) + 6.0 * (a + b + c)),
            forc[i].astype(F32),
        )
        ix_s[i], iy_s[i], iz_s[i], rd_s[i], _ = values
        return tuple(into_strip(i, v, strip) for v, strip in zip(values, strips))

    strips = lax.fori_loop(0, n, coefficient, (zero,) * 5, unroll=8)
    for k in range(5):
        tb[k] = strips[k]

    def vertical(i, ref):
        return ref[i, pl.ds(0, levels), :], ref[i, pl.ds(1, levels), :]

    def collect(fields):
        fx, fy, fz = fields

        def body(i, strips):
            y = fy[i]
            b, t = vertical(i, fz)
            return (
                into_strip(i, fx[i], strips[0]),
                into_strip(i, y, strips[1]),
                lane1_into_strip(i, y, strips[2]),
                into_strip(i, b, strips[3]),
                into_strip(i, t, strips[4]),
            )

        strips = lax.fori_loop(0, n, body, (zero,) * 5, unroll=8)
        for k in range(5):
            tb[5 + k] = strips[k]

    def row(i, fields, strip, fresh, source):
        fx, fy, fz = fields
        edge = pltpu.roll(strip, m - 1 - 2 * i, 1)
        s = fy[i]
        if not fresh:
            s = s + jnp.where(lane == 0, edge, 0.0)
        north_side = jnp.where(lane == m - 1, edge, pltpu.roll(s, m - 1, 1))
        b, t = vertical(i, fz)
        w, e = fx[i], fx[i + 1]
        g = forc[i].astype(F32) if source else None
        flux, p = cell(w, e, s, north_side, b, t, ix_s[i], iy_s[i], iz_s[i], rd_s[i], g)
        return (w, e, s, north_side, b, t), flux, p

    def send_boundary(base, fields, strip, fresh, source, sign):
        fx = fields[0]
        last = pltpu.roll(fx[n], 2 * n - 1, 1)
        tw = tb[5]
        te = jnp.where(pair == n - 1, last, pltpu.roll(tw, m - 2, 1))
        ts = tb[6]
        if not fresh:
            tw = jnp.where(pair == 0, pltpu.roll(fx[0], 1, 1), tw)
            ts = ts + jnp.where(odd, strip, 0.0)
            tb[10] = ts
        tn = jnp.where(odd, tb[7], strip)
        flux, _ = cell(
            tw, te, ts, tn, tb[8], tb[9], tb[0], tb[1], tb[2], tb[3], tb[4] if source else None
        )
        send_b[base + 2] = sign * jnp.where(odd, flux[2], flux[3])
        send_b[base] = sign * row(0, fields, strip, fresh, source)[1][0]
        send_b[base + 1] = sign * row(n - 1, fields, strip, fresh, source)[1][1]
        copies = [
            exchange(base + 2, base + 2, south),
            exchange(base + 2, base + 3, north),
            exchange(base, base, west),
            exchange(base + 1, base + 1, east),
        ]
        for copy in copies:
            copy.start()
        return copies

    def arrive(base, copies, out_x):
        for copy in copies:
            copy.wait_recv()
        out_x[0] = out_x[0] + recv_b[base + 1]
        out_x[n] = out_x[n] + recv_b[base]
        high = send_b[base + 2] + pltpu.roll(recv_b[base + 2], m - 1, 1)
        return jnp.where(odd, pltpu.roll(recv_b[base + 3], 1, 1), high)

    def assemble(i, flux, fe_before, outs, sign):
        fw, fe, fs, fn, fb, ft = flux
        out_x, out_y, out_z = outs
        out_x[i] = sign * (fw + fe_before)
        out_y[i] = sign * (fs + jnp.where(lane == 0, 0.0, pltpu.roll(fn, 1, 1)))
        shifted = pltpu.roll(ft, 1, 0)
        out_z[i, pl.ds(0, levels), :] = sign * (fb + jnp.where(level == 0, 0.0, shifted))
        out_z[i, pl.ds(levels, 1), :] = sign * shifted[0:1]
        return fe

    start = (x_ref, y_ref, z_x)
    residual = (rx, ry, rz_x)
    image = (wx, wy, wz_x)

    def turn(i, carry):
        z_x[i] = z_ref[pl.ds(i, levels + 1, stride=n), :]
        return carry

    lax.fori_loop(0, n, turn, 0, unroll=4)
    collect(start)
    for copy in first:
        copy.wait_recv()
    x_ref[n] = recv_b[0]
    strip = pltpu.roll(recv_b[1], m - 1, 1)
    copies1 = send_boundary(2, start, strip, True, True, -1.0)

    def pass1(i, fe_before):
        _, flux, p = row(i, start, strip, True, True)
        p0[i] = p
        return assemble(i, flux, fe_before, residual, -1.0)

    rx[n] = -lax.fori_loop(0, n, pass1, zero, unroll=8)
    collect(residual)

    strip2 = arrive(2, copies1, rx)
    copies2 = send_boundary(6, residual, strip2, False, False, 1.0)

    def pass2(i, carry):
        fe_before, rr = carry
        (w, e, s, north_side, b, t), flux, p = row(i, residual, strip2, False, False)
        ry[i] = s
        p1[i] = p
        top = jnp.where(level == levels - 1, t, 0.0)
        rr = rr + (w * w + s * s + b * b + top * top)
        return assemble(i, flux, fe_before, image, 1.0), rr

    wx[n], rr = lax.fori_loop(0, n, pass2, (zero, zero), unroll=8)

    collect(image)

    inner = jnp.logical_and(lane > 0, lane < m - 1)

    def quadratic(faces, flux):
        w, e, s, north_side, b, t = faces
        fw, fe, fs, fn, fb, ft = flux
        return (w * fw + e * fe) + (s * fs + north_side * fn) + (b * fb + t * ft)

    def pass3(i, carry):
        rw, ww, waw = carry
        s = wy[i]
        north_side = pltpu.roll(s, m - 1, 1)
        b, t = vertical(i, wz_x)
        rb, rt = vertical(i, rz_x)
        w, e = wx[i], wx[i + 1]
        flux, _ = cell(w, e, s, north_side, b, t, ix_s[i], iy_s[i], iz_s[i], rd_s[i], None)
        between = jnp.logical_and(i > 0, i < n - 1)
        sm = jnp.where(lane == 0, 0.0, s)
        top = jnp.where(level == levels - 1, t, 0.0)
        rw = rw + jnp.where(between, w * rx[i] + sm * ry[i] + b * rb + top * rt, 0.0)
        ww = ww + jnp.where(between, w * w + sm * sm + b * b + top * top, 0.0)
        kept = jnp.logical_and(inner, between)
        waw = waw + jnp.where(kept, quadratic((w, e, s, north_side, b, t), flux), 0.0)
        return rw, ww, waw

    rw, ww, waw = lax.fori_loop(0, n, pass3, (zero, zero, zero), unroll=8)

    strip3 = arrive(6, copies2, wx)
    rest_of = jnp.logical_and(pair > 0, pair < n - 1)
    tw, ts = tb[5], tb[6] + jnp.where(odd, strip3, 0.0)
    te, tn = pltpu.roll(tw, m - 2, 1), jnp.where(odd, tb[7], strip3)
    faces = (tw, te, ts, tn, tb[8], tb[9])
    flux, _ = cell(*faces, tb[0], tb[1], tb[2], tb[3], None)
    waw = waw + jnp.where(rest_of, quadratic(faces, flux), 0.0)
    ts = jnp.where(jnp.logical_and(rest_of, odd), ts, 0.0)
    ww = ww + ts * ts
    rw = rw + ts * tb[10]
    for i in (0, n - 1):
        faces, flux, _ = row(i, image, strip3, False, False)
        w, _, s, _, b, t = faces
        rb, rt = vertical(i, rz_x)
        top = jnp.where(level == levels - 1, t, 0.0)
        rw = rw + (w * rx[i] + s * ry[i] + b * rb + top * rt)
        ww = ww + (w * w + s * s + b * b + top * top)
        waw = waw + quadratic(faces, flux)

    def finish(i, carry):
        faces, _, p = row(i, image, strip3, False, False)
        wy[i] = faces[2]
        p2[i] = p
        rz[pl.ds(i, levels + 1, stride=n), :] = rz_x[i]
        wz[pl.ds(i, levels + 1, stride=n), :] = wz_x[i]
        return carry

    lane_row = lax.broadcasted_iota(jnp.int32, (1, m), 1)
    sums = jnp.zeros((1, m), F32)
    for k, part in enumerate((rr, rw, ww, waw)):
        whole = jnp.sum(jnp.sum(part, axis=0, keepdims=True), axis=1, keepdims=True)
        sums = jnp.where(lane_row == k, whole, sums)

    for k, (group, slot) in enumerate(zip(groups, slots)):
        row_b[k] = sums
        for j, device in enumerate(group):
            pltpu.make_async_remote_copy(
                src_ref=row_b.at[pl.ds(k, 1)],
                dst_ref=slot.at[pl.ds(j, 1)],
                send_sem=ar_send.at[k],
                recv_sem=ar_recv.at[k],
                device_id=device,
                device_id_type=MESH,
            ).start()
        if k == 0:
            lax.fori_loop(0, n, finish, 0, unroll=4)
        everything = pltpu.make_async_remote_copy(
            src_ref=slot, dst_ref=slot, send_sem=ar_send.at[k], recv_sem=ar_recv.at[k],
            device_id=group[0], device_id_type=MESH,
        )
        everything.wait_recv()
        sums = sums + jnp.sum(slot[...], axis=0)
        everything.wait_send()

    rr, rw, ww, waw = [
        jnp.sum(jnp.where(lane_row == k, sums, 0.0), axis=1, keepdims=True) for k in range(4)
    ]
    a0 = rr / rw
    grown = ww * a0 / rw
    b = grown - 1.0
    a1 = b * rr / (a0 * a0 * waw - grown * grown * rw)
    coef[0] = jnp.broadcast_to(a0 + a1 * grown, coef.shape[1:])
    coef[1] = jnp.broadcast_to(-a1 * a0, coef.shape[1:])
    for copy in first + copies1 + copies2:
        copy.wait_send()


def combine_kernel(
    x_ref, y_ref, z_ref, rx, ry, rz, wx, wy, wz, p0, p1, p2, coef,
    ox_h, oy_h, oz_h, op_h, ox, oy, oz, op, sem,
):
    n = ox.shape[0]
    chunks = 5
    rows = n // chunks
    step = n
    c1, c2 = coef[0, 0:1, :], coef[1, 0:1, :]
    copies = []
    for k in range(chunks):

        def body(i, carry):
            ox[i] = x_ref[i] + (c1 * rx[i] + c2 * wx[i])
            oy[i] = y_ref[i] + (c1 * ry[i] + c2 * wy[i])
            op[i] = p0[i] + (c1 * p1[i] + c2 * p2[i])
            return carry

        lax.fori_loop(k * rows, (k + 1) * rows, body, 0)
        tall = oz.shape[0] // chunks

        def body_z(i, carry):
            at = pl.ds(pl.multiple_of(i * step, step), step)
            oz[at, :] = z_ref[at, :] + (c1 * rz[at, :] + c2 * wz[at, :])
            return carry

        lax.fori_loop(k * (tall // step), (k + 1) * (tall // step), body_z, 0)
        span = pl.ds(k * rows, rows)
        span_z = pl.ds(k * tall, tall)
        for j, (src, dst, at) in enumerate(
            ((ox, ox_h, span), (oy, oy_h, span), (oz, oz_h, span_z), (op, op_h, span))
        ):
            copy = pltpu.make_async_copy(src.at[at], dst.at[at], sem.at[k, j])
            copy.start()
            copies.append(copy)
    for copy in copies:
        copy.wait()


def local(px, py, metric, helmholtz, forcing, orientation, start_x, start_y, start_z):
    n, levels, m = helmholtz.shape
    face = (n, levels, m)
    longer = (n + 1, levels, m)
    taller = ((levels + 1) * n, m)
    start_z = jnp.transpose(start_z, (1, 0, 2)).reshape(taller)
    arguments = [
        pltpu.with_memory_space_constraint(a, pltpu.HBM)
        for a in (metric, helmholtz, forcing, orientation, start_x, start_y, start_z)
    ]
    shapes = [longer, face, taller, longer, face, taller, longer, face, taller, face, face, face, (2, 8, m)]
    held = pl.pallas_call(
        functools.partial(halo_kernel, px, py),
        out_shape=[pltpu.VMEM(shape, F32) for shape in shapes],
        in_specs=[pl.BlockSpec(memory_space=pl.ANY)] * 7,
        out_specs=[pl.BlockSpec(memory_space=pltpu.VMEM)] * len(shapes),
        scratch_shapes=[
            pltpu.VMEM((3,) + face, metric.dtype),
            pltpu.VMEM(face, helmholtz.dtype),
            pltpu.VMEM(face, forcing.dtype),
            pltpu.VMEM((n, m), jnp.int32),
            pltpu.VMEM(face, F32),
            pltpu.VMEM(face, F32),
            pltpu.VMEM(face, F32),
            pltpu.VMEM(face, F32),
            pltpu.VMEM((n, levels + 1, m), F32),
            pltpu.VMEM((n, levels + 1, m), F32),
            pltpu.VMEM((n, levels + 1, m), F32),
            pltpu.VMEM((11, levels, m), F32),
            pltpu.VMEM((10, levels, m), F32),
            pltpu.VMEM((10, levels, m), F32),
            pltpu.VMEM((len(PHASES), 1, m), F32),
        ]
        + [pltpu.VMEM((group_size(px, py, dims) - 1, 1, m), F32) for dims in PHASES]
        + [
            pltpu.SemaphoreType.DMA((7,)),
            pltpu.SemaphoreType.DMA((10,)),
            pltpu.SemaphoreType.DMA((10,)),
            pltpu.SemaphoreType.DMA((len(PHASES),)),
            pltpu.SemaphoreType.DMA((len(PHASES),)),
        ],
        compiler_params=pltpu.CompilerParams(
            collective_id=0, has_side_effects=True, vmem_limit_bytes=40 * 1024 * 1024
        ),
        name="halo",
    )(*arguments)
    outs = [face, face, taller, face]
    trace_x, trace_y, trace_z, pressure = pl.pallas_call(
        combine_kernel,
        out_shape=[jax.ShapeDtypeStruct(shape, F32) for shape in outs],
        in_specs=[pl.BlockSpec(memory_space=pltpu.VMEM)] * len(shapes),
        out_specs=[pl.BlockSpec(memory_space=pl.ANY)] * 4,
        scratch_shapes=[pltpu.VMEM(shape, F32) for shape in outs]
        + [pltpu.SemaphoreType.DMA((5, 4))],
        compiler_params=pltpu.CompilerParams(vmem_limit_bytes=20 * 1024 * 1024),
        name="combine",
    )(*held)
    trace_z = jnp.transpose(trace_z.reshape(levels + 1, n, m), (1, 0, 2))
    return trace_x, trace_y, trace_z, pressure


def solution(mesh):
    px, py = mesh.shape["px"], mesh.shape["py"]
    columns = P("px", None, "py")
    return jax.shard_map(
        functools.partial(local, px, py),
        mesh=mesh,
        in_specs=(P(None, "px", None, "py"), columns, columns, P("px", "py"), columns, columns, columns),
        out_specs=(columns,) * 4,
        check_vma=False,
    )
```

```python
import functools
import itertools

import jax
import jax.numpy as jnp
from jax import lax
from jax.experimental import pallas as pl
from jax.experimental.pallas import tpu as pltpu
from jax.sharding import PartitionSpec as P

MESH = pl.DeviceIdType.MESH
F32 = jnp.float32


def factors(px, py):
    if px == 16 and py == 32:
        return (2, 4, 2), (4, 8)
    return (1, px // 2, 2), (2, py // 2)


def peers(px, py, me_x, me_y, dims):
    (ny_lo, nx, nc), (ny_hi, nz) = factors(px, py)
    sizes = {"y_lo": ny_lo, "x": nx, "core": nc, "y_hi": ny_hi, "z": nz}
    here = {
        "core": lax.rem(me_x, nc),
        "x": lax.rem(me_x // nc, nx),
        "y_lo": me_x // (nc * nx),
        "z": lax.rem(me_y, nz),
        "y_hi": me_y // nz,
    }
    reach = {"core": 0, "x": 1, "y_lo": 1, "z": 1, "y_hi": 2}

    def far(offset):
        return sum(reach[d] * min(o, sizes[d] - o) for d, o in zip(dims, offset))

    found = []
    offsets = itertools.product(*[range(sizes[d]) for d in dims])
    for offset in sorted(offsets, key=far, reverse=True):
        if not any(offset):
            continue
        there = dict(here)
        for d, o in zip(dims, offset):
            there[d] = lax.rem(here[d] + o, sizes[d])
        found.append(
            {
                "px": (there["y_lo"] * nx + there["x"]) * nc + there["core"],
                "py": there["y_hi"] * nz + there["z"],
            }
        )
    return found


PHASES = (("core", "z"), ("x", "y_lo", "y_hi"))


def group_size(px, py, dims):
    (ny_lo, nx, nc), (ny_hi, nz) = factors(px, py)
    sizes = {"y_lo": ny_lo, "x": nx, "core": nc, "y_hi": ny_hi, "z": nz}
    total = 1
    for d in dims:
        total *= sizes[d]
    return total


def cell(w, e, s, n, b, t, ix, iy, iz, rd, g):
    sx, sy, sz = w + e, s + n, b + t
    total = 3.0 * (ix * sx + iy * sy + iz * sz)
    if g is not None:
        total = total + g
    p = total * rd
    p3 = 3.0 * p
    qx, qy, qz = sx - p3, sy - p3, sz - p3
    return (
        (ix * (qx + w), ix * (qx + e), iy * (qy + s), iy * (qy + n), iz * (qz + b), iz * (qz + t)),
        p,
    )


def halo_kernel(
    px, py,
    metric_h, helm_h, forc_h, orient_h, sx_h, sy_h, sz_h,
    x_ref, y_ref, z_ref, rx, ry, rz, wx, wy, wz, p0, p1, p2, coef,
    metric, helm, forc, orient, ix_s, iy_s, iz_s, rd_s,
    z_x, rz_x, wz_x, tb, send_b, recv_b, msg_s, msg_r, dia_s, dia_r, row_b, *rest,
):
    slots = rest[: len(PHASES)]
    load_sem, send_sem, recv_sem, ar_send, ar_recv = rest[len(PHASES) :]
    n, levels, m = helm.shape
    me_x, me_y = lax.axis_index("px"), lax.axis_index("py")
    west = {"px": lax.rem(me_x + px - 1, px), "py": me_y}
    east = {"px": lax.rem(me_x + 1, px), "py": me_y}
    south = {"px": me_x, "py": lax.rem(me_y + py - 1, py)}
    north = {"px": me_x, "py": lax.rem(me_y + 1, py)}
    corner = [
        {"px": x["px"], "py": y["py"]} for x in (east, west) for y in (north, south)
    ]
    groups = [peers(px, py, me_x, me_y, dims) for dims in PHASES]

    loads = [
        pltpu.make_async_copy(src, dst, load_sem.at[k])
        for k, (src, dst) in enumerate(
            [
                (sy_h, y_ref),
                (sx_h, x_ref.at[pl.ds(0, n)]),
                (metric_h, metric),
                (orient_h, orient),
                (helm_h, helm),
                (forc_h, forc),
                (sz_h, z_ref),
            ]
        )
    ]
    for load in loads:
        load.start()

    barrier = pltpu.get_barrier_semaphore()
    greeted = [west, east, south, north] + corner + [d for group in groups for d in group]
    for device in greeted:
        pl.semaphore_signal(barrier, inc=1, device_id=device, device_id_type=MESH)

    lane = lax.broadcasted_iota(jnp.int32, (levels, m), 1)
    level = lax.broadcasted_iota(jnp.int32, (levels, m), 0)
    pair = jnp.right_shift(lane, 1)
    odd = jnp.bitwise_and(lane, 1) == 1
    zero = jnp.zeros((levels, m), F32)

    def into_strip(i, value, strip):
        return jnp.where(pair == i, pltpu.roll(value, 2 * i + 1, 1), strip)

    def lane1_into_strip(i, value, strip):
        return jnp.where(lane == 2 * i + 1, pltpu.roll(value, 2 * i, 1), strip)

    def exchange(source, target, slot, device):
        return pltpu.make_async_remote_copy(
            src_ref=source,
            dst_ref=target,
            send_sem=send_sem.at[slot],
            recv_sem=recv_sem.at[slot],
            device_id=device,
            device_id_type=MESH,
        )

    for load in loads:
        load.wait()

    def coefficient(i, strips):
        a = 1.0 / metric[0, i].astype(F32)
        b = 1.0 / metric[1, i].astype(F32)
        c = 1.0 / metric[2, i].astype(F32)
        turned = orient[pl.ds(i, 1), :] == 1
        values = (
            jnp.where(turned, b, a),
            jnp.where(turned, a, b),
            c,
            1.0 / (helm[i].astype(F32) + 6.0 * (a + b + c)),
            forc[i].astype(F32),
        )
        ix_s[i], iy_s[i], iz_s[i], rd_s[i], _ = values
        return tuple(into_strip(i, v, strip) for v, strip in zip(values, strips))

    strips = lax.fori_loop(0, n, coefficient, (zero,) * 5, unroll=8)
    for k in range(5):
        tb[k] = strips[k]

    def vertical(i, ref):
        return ref[i, pl.ds(0, levels), :], ref[i, pl.ds(1, levels), :]

    def collect(fields, base):
        fx, fy, fz = fields

        def body(i, strips):
            y = fy[i]
            b, t = vertical(i, fz)
            return (
                into_strip(i, fx[i], strips[0]),
                into_strip(i, y, strips[1]),
                lane1_into_strip(i, y, strips[2]),
                into_strip(i, b, strips[3]),
                into_strip(i, t, strips[4]),
            )

        strips = lax.fori_loop(0, n, body, (zero,) * 5, unroll=8)
        for k in range(5):
            tb[base + k] = strips[k]

    def row(i, fields, strip, fresh, source):
        fx, fy, fz = fields
        edge = pltpu.roll(strip, m - 1 - 2 * i, 1)
        s = fy[i]
        if not fresh:
            s = s + jnp.where(lane == 0, edge, 0.0)
        north_side = jnp.where(lane == m - 1, edge, pltpu.roll(s, m - 1, 1))
        b, t = vertical(i, fz)
        w, e = fx[i], fx[i + 1]
        g = forc[i].astype(F32) if source else None
        flux, p = cell(w, e, s, north_side, b, t, ix_s[i], iy_s[i], iz_s[i], rd_s[i], g)
        return (w, e, s, north_side, b, t), flux, p

    def strip_flux(base, last, strip, source):
        te = jnp.where(pair == n - 1, pltpu.roll(last, 2 * n - 1, 1), pltpu.roll(tb[base], m - 2, 1))
        tn = jnp.where(odd, tb[base + 2], strip)
        return cell(
            tb[base], te, tb[base + 1], tn, tb[base + 3], tb[base + 4],
            tb[0], tb[1], tb[2], tb[3], tb[4] if source else None,
        )[0]

    def assemble(i, flux, fe_before, outs, sign):
        fw, fe, fs, fn, fb, ft = flux
        out_x, out_y, out_z = outs
        out_x[i] = sign * (fw + fe_before)
        out_y[i] = sign * (fs + jnp.where(lane == 0, 0.0, pltpu.roll(fn, 1, 1)))
        shifted = pltpu.roll(ft, 1, 0)
        out_z[i, pl.ds(0, levels), :] = sign * (fb + jnp.where(level == 0, 0.0, shifted))
        out_z[i, pl.ds(levels, 1), :] = sign * shifted[0:1]
        return fe

    start = (x_ref, y_ref, z_x)
    residual = (rx, ry, rz_x)
    image = (wx, wy, wz_x)

    def turn(i, carry):
        z_x[i] = z_ref[pl.ds(i, levels + 1, stride=n), :]
        return carry

    lax.fori_loop(0, n, turn, 0, unroll=4)
    x_ref[n] = zero
    collect(start, 5)

    flux = strip_flux(5, zero, zero, True)
    both = 9.0 * tb[0] * tb[1] * tb[3]
    msg_s[2, 0] = tb[6]
    msg_s[2, 1] = -flux[2]
    msg_s[2, 2] = both
    msg_s[3, 0] = -flux[3]
    msg_s[3, 1] = 9.0 * tb[1] * tb[1] * tb[3] - 2.0 * tb[1]
    msg_s[3, 2] = both
    msg_s[0, 0] = x_ref[0]
    msg_s[0, 1] = -row(0, start, zero, True, True)[1][0]
    msg_s[0, 2] = 9.0 * ix_s[0] * iy_s[0] * rd_s[0]
    msg_s[1, 0] = -row(n - 1, start, zero, True, True)[1][1]
    msg_s[1, 1] = 9.0 * ix_s[n - 1] * ix_s[n - 1] * rd_s[n - 1] - 2.0 * ix_s[n - 1]
    msg_s[1, 2] = 9.0 * ix_s[n - 1] * iy_s[n - 1] * rd_s[n - 1]
    dia_s[0] = jnp.where(
        lane == m - 1, pltpu.roll(y_ref[0], m - 1, 1), pltpu.roll(x_ref[0], 2 * n - 1, 1)
    )
    dia_s[1] = pltpu.roll(y_ref[n - 1], m - 1, 1)
    north_east, south_east, north_west, south_west = corner
    first = [
        exchange(dia_s.at[0], dia_r.at[0], 8, south_west),
        exchange(dia_s.at[0], dia_r.at[1], 9, north_west),
        exchange(dia_s.at[1], dia_r.at[2], 10, south_east),
    ] + [
        exchange(msg_s.at[k], msg_r.at[k], 4 + k, device)
        for k, device in ((2, south), (3, north), (0, west), (1, east))
    ]
    pl.semaphore_wait(barrier, len(greeted))
    for copy in first:
        copy.start()

    def pass1(i, fe_before):
        _, flux, _ = row(i, start, zero, True, True)
        return assemble(i, flux, fe_before, residual, -1.0)

    lax.fori_loop(0, n, pass1, zero, unroll=8)
    collect(residual, 11)

    for copy in first:
        copy.wait_recv()
    x_ref[n] = msg_r[0, 0]
    strip1 = pltpu.roll(msg_r[2, 0], m - 1, 1)
    from_east = msg_r[0, 1] + jnp.where(lane == m - 1, msg_r[0, 2] * dia_r[0], 0.0)
    from_west = (
        msg_r[1, 0]
        + msg_r[1, 1] * x_ref[0]
        + jnp.where(lane == m - 1, msg_r[1, 2] * dia_r[2], 0.0)
    )
    from_north = msg_r[2, 1] + jnp.where(lane == 2 * n - 1, msg_r[2, 2] * dia_r[0], 0.0)
    from_south = (
        msg_r[3, 0]
        + msg_r[3, 1] * pltpu.roll(tb[6], m - 1, 1)
        + jnp.where(lane == 2 * n - 2, msg_r[3, 2] * dia_r[1], 0.0)
    )
    high = pltpu.roll(from_north, m - 1, 1) - strip_flux(5, x_ref[n], strip1, True)[3]
    strip2 = jnp.where(odd, pltpu.roll(from_south, 1, 1), high)

    own = jnp.where(odd, 0.0, strip1)
    dp = 3.0 * tb[1] * tb[3] * own
    dx, dz = 3.0 * tb[0] * dp, 3.0 * tb[2] * dp
    add_x = dx + pltpu.roll(dx, 2, 1)
    add_y = 3.0 * tb[1] * dp - tb[1] * own
    add_b = dz + jnp.where(level == 0, 0.0, pltpu.roll(dz, 1, 0))
    add_t = dz + jnp.where(level == levels - 1, 0.0, pltpu.roll(dz, levels - 1, 0))

    f0 = row(0, start, strip1, True, True)[1]
    assemble(0, f0, -from_west, residual, -1.0)
    assemble(1, row(1, start, strip1, True, True)[1], f0[1], residual, -1.0)
    before = row(n - 2, start, strip1, True, True)[1][1]
    fe_last = assemble(n - 1, row(n - 1, start, strip1, True, True)[1], before, residual, -1.0)
    rx[n] = from_east - fe_last
    b_last, t_last = vertical(n - 1, rz_x)
    tb[11] = into_strip(0, rx[0], into_strip(n - 1, rx[n - 1], tb[11] + add_x))
    tb[12] = into_strip(n - 1, ry[n - 1], tb[12] + add_y) + jnp.where(odd, strip2, 0.0)
    tb[13] = lane1_into_strip(n - 1, ry[n - 1], tb[13])
    tb[14] = into_strip(n - 1, b_last, tb[14] + add_b)
    tb[15] = into_strip(n - 1, t_last, tb[15] + add_t)

    flux = strip_flux(11, rx[n], strip2, False)
    send_b[2] = jnp.where(odd, flux[2], flux[3])
    send_b[0] = row(0, residual, strip2, False, False)[1][0]
    send_b[1] = row(n - 1, residual, strip2, False, False)[1][1]
    second = [
        exchange(send_b.at[2], recv_b.at[2], 2, south),
        exchange(send_b.at[2], recv_b.at[3], 3, north),
        exchange(send_b.at[0], recv_b.at[0], 0, west),
        exchange(send_b.at[1], recv_b.at[1], 1, east),
    ]
    for copy in second:
        copy.start()

    rows_left = jnp.logical_and(pair > 1, pair < n - 1)
    adds = [jnp.where(rows_left, a, 0.0) for a in (add_x, add_y, add_b, add_t)]

    def amend(i, carry):
        ax, ay, ab, at = [
            jnp.where(lane == m - 1, pltpu.roll(a, m - 1 - 2 * i, 1), 0.0) for a in adds
        ]
        rx[i] = rx[i] + ax
        ry[i] = ry[i] + ay
        rz_x[i, pl.ds(0, levels), :] = rz_x[i, pl.ds(0, levels), :] + ab
        top = pl.ds(levels, 1)
        rz_x[i, top, :] = rz_x[i, top, :] + at[levels - 1 :]
        return carry

    lax.fori_loop(0, n, amend, 0, unroll=8)

    def pass2(i, carry):
        fe_before, rr = carry
        (w, e, s, north_side, b, t), flux, p = row(i, residual, strip2, False, False)
        ry[i] = s
        p1[i] = p
        top = jnp.where(level == levels - 1, t, 0.0)
        rr = rr + (w * w + s * s + b * b + top * top)
        return assemble(i, flux, fe_before, image, 1.0), rr

    wx[n], rr = lax.fori_loop(0, n, pass2, (zero, zero), unroll=8)

    collect(image, 5)

    inner = jnp.logical_and(lane > 0, lane < m - 1)

    def quadratic(faces, flux):
        w, e, s, north_side, b, t = faces
        fw, fe, fs, fn, fb, ft = flux
        return (w * fw + e * fe) + (s * fs + north_side * fn) + (b * fb + t * ft)

    def pass3(i, carry):
        rw, ww, waw = carry
        s = wy[i]
        north_side = pltpu.roll(s, m - 1, 1)
        b, t = vertical(i, wz_x)
        rb, rt = vertical(i, rz_x)
        w, e = wx[i], wx[i + 1]
        flux, _ = cell(w, e, s, north_side, b, t, ix_s[i], iy_s[i], iz_s[i], rd_s[i], None)
        between = jnp.logical_and(i > 0, i < n - 1)
        sm = jnp.where(lane == 0, 0.0, s)
        top = jnp.where(level == levels - 1, t, 0.0)
        rw = rw + jnp.where(between, w * rx[i] + sm * ry[i] + b * rb + top * rt, 0.0)
        ww = ww + jnp.where(between, w * w + sm * sm + b * b + top * top, 0.0)
        kept = jnp.logical_and(inner, between)
        waw = waw + jnp.where(kept, quadratic((w, e, s, north_side, b, t), flux), 0.0)
        return rw, ww, waw

    rw, ww, waw = lax.fori_loop(0, n, pass3, (zero, zero, zero), unroll=8)

    for copy in second:
        copy.wait_recv()
    wx[0] = wx[0] + recv_b[1]
    wx[n] = wx[n] + recv_b[0]
    high = send_b[2] + pltpu.roll(recv_b[2], m - 1, 1)
    strip3 = jnp.where(odd, pltpu.roll(recv_b[3], 1, 1), high)
    rest_of = jnp.logical_and(pair > 0, pair < n - 1)
    tw, ts = tb[5], tb[6] + jnp.where(odd, strip3, 0.0)
    te, tn = pltpu.roll(tw, m - 2, 1), jnp.where(odd, tb[7], strip3)
    faces = (tw, te, ts, tn, tb[8], tb[9])
    flux, _ = cell(*faces, tb[0], tb[1], tb[2], tb[3], None)
    waw = waw + jnp.where(rest_of, quadratic(faces, flux), 0.0)
    ts = jnp.where(jnp.logical_and(rest_of, odd), ts, 0.0)
    ww = ww + ts * ts
    rw = rw + ts * tb[12]
    for i in (0, n - 1):
        faces, flux, _ = row(i, image, strip3, False, False)
        w, _, s, _, b, t = faces
        rb, rt = vertical(i, rz_x)
        top = jnp.where(level == levels - 1, t, 0.0)
        rw = rw + (w * rx[i] + s * ry[i] + b * rb + top * rt)
        ww = ww + (w * w + s * s + b * b + top * top)
        waw = waw + quadratic(faces, flux)

    def finish(i, carry):
        faces, _, p = row(i, image, strip3, False, False)
        wy[i] = faces[2]
        p2[i] = p
        p0[i] = row(i, start, strip1, True, True)[2]
        rz[pl.ds(i, levels + 1, stride=n), :] = rz_x[i]
        wz[pl.ds(i, levels + 1, stride=n), :] = wz_x[i]
        return carry

    lane_row = lax.broadcasted_iota(jnp.int32, (1, m), 1)
    sums = jnp.zeros((1, m), F32)
    for k, part in enumerate((rr, rw, ww, waw)):
        whole = jnp.sum(jnp.sum(part, axis=0, keepdims=True), axis=1, keepdims=True)
        sums = jnp.where(lane_row == k, whole, sums)

    for k, (group, slot) in enumerate(zip(groups, slots)):
        row_b[k] = sums
        for j, device in enumerate(group):
            pltpu.make_async_remote_copy(
                src_ref=row_b.at[pl.ds(k, 1)],
                dst_ref=slot.at[pl.ds(j, 1)],
                send_sem=ar_send.at[k],
                recv_sem=ar_recv.at[k],
                device_id=device,
                device_id_type=MESH,
            ).start()
        if k == 0:
            lax.fori_loop(0, n, finish, 0, unroll=4)
        everything = pltpu.make_async_remote_copy(
            src_ref=slot, dst_ref=slot, send_sem=ar_send.at[k], recv_sem=ar_recv.at[k],
            device_id=group[0], device_id_type=MESH,
        )
        everything.wait_recv()
        sums = sums + jnp.sum(slot[...], axis=0)
        everything.wait_send()

    rr, rw, ww, waw = [
        jnp.sum(jnp.where(lane_row == k, sums, 0.0), axis=1, keepdims=True) for k in range(4)
    ]
    a0 = rr / rw
    grown = ww * a0 / rw
    b = grown - 1.0
    a1 = b * rr / (a0 * a0 * waw - grown * grown * rw)
    coef[0] = jnp.broadcast_to(a0 + a1 * grown, coef.shape[1:])
    coef[1] = jnp.broadcast_to(-a1 * a0, coef.shape[1:])
    for copy in first + second:
        copy.wait_send()


def combine_kernel(
    x_ref, y_ref, z_ref, rx, ry, rz, wx, wy, wz, p0, p1, p2, coef,
    ox_h, oy_h, oz_h, op_h, ox, oy, oz, op, sem,
):
    n = ox.shape[0]
    chunks = 5
    rows = n // chunks
    step = n
    c1, c2 = coef[0, 0:1, :], coef[1, 0:1, :]
    copies = []
    for k in range(chunks):

        def body(i, carry):
            ox[i] = x_ref[i] + (c1 * rx[i] + c2 * wx[i])
            oy[i] = y_ref[i] + (c1 * ry[i] + c2 * wy[i])
            op[i] = p0[i] + (c1 * p1[i] + c2 * p2[i])
            return carry

        lax.fori_loop(k * rows, (k + 1) * rows, body, 0)
        tall = oz.shape[0] // chunks

        def body_z(i, carry):
            at = pl.ds(pl.multiple_of(i * step, step), step)
            oz[at, :] = z_ref[at, :] + (c1 * rz[at, :] + c2 * wz[at, :])
            return carry

        lax.fori_loop(k * (tall // step), (k + 1) * (tall // step), body_z, 0)
        span = pl.ds(k * rows, rows)
        span_z = pl.ds(k * tall, tall)
        for j, (src, dst, at) in enumerate(
            ((ox, ox_h, span), (oy, oy_h, span), (oz, oz_h, span_z), (op, op_h, span))
        ):
            copy = pltpu.make_async_copy(src.at[at], dst.at[at], sem.at[k, j])
            copy.start()
            copies.append(copy)
    for copy in copies:
        copy.wait()


def local(px, py, metric, helmholtz, forcing, orientation, start_x, start_y, start_z):
    n, levels, m = helmholtz.shape
    face = (n, levels, m)
    longer = (n + 1, levels, m)
    taller = ((levels + 1) * n, m)
    start_z = jnp.transpose(start_z, (1, 0, 2)).reshape(taller)
    arguments = [
        pltpu.with_memory_space_constraint(a, pltpu.HBM)
        for a in (metric, helmholtz, forcing, orientation, start_x, start_y, start_z)
    ]
    shapes = [longer, face, taller, longer, face, taller, longer, face, taller, face, face, face, (2, 8, m)]
    held = pl.pallas_call(
        functools.partial(halo_kernel, px, py),
        out_shape=[pltpu.VMEM(shape, F32) for shape in shapes],
        in_specs=[pl.BlockSpec(memory_space=pl.ANY)] * 7,
        out_specs=[pl.BlockSpec(memory_space=pltpu.VMEM)] * len(shapes),
        scratch_shapes=[
            pltpu.VMEM((3,) + face, metric.dtype),
            pltpu.VMEM(face, helmholtz.dtype),
            pltpu.VMEM(face, forcing.dtype),
            pltpu.VMEM((n, m), jnp.int32),
            pltpu.VMEM(face, F32),
            pltpu.VMEM(face, F32),
            pltpu.VMEM(face, F32),
            pltpu.VMEM(face, F32),
            pltpu.VMEM((n, levels + 1, m), F32),
            pltpu.VMEM((n, levels + 1, m), F32),
            pltpu.VMEM((n, levels + 1, m), F32),
            pltpu.VMEM((16, levels, m), F32),
            pltpu.VMEM((3, levels, m), F32),
            pltpu.VMEM((4, levels, m), F32),
            pltpu.VMEM((4, 3, levels, m), F32),
            pltpu.VMEM((4, 3, levels, m), F32),
            pltpu.VMEM((2, levels, m), F32),
            pltpu.VMEM((3, levels, m), F32),
            pltpu.VMEM((len(PHASES), 1, m), F32),
        ]
        + [pltpu.VMEM((group_size(px, py, dims) - 1, 1, m), F32) for dims in PHASES]
        + [
            pltpu.SemaphoreType.DMA((7,)),
            pltpu.SemaphoreType.DMA((11,)),
            pltpu.SemaphoreType.DMA((11,)),
            pltpu.SemaphoreType.DMA((len(PHASES),)),
            pltpu.SemaphoreType.DMA((len(PHASES),)),
        ],
        compiler_params=pltpu.CompilerParams(
            collective_id=0, has_side_effects=True, vmem_limit_bytes=40 * 1024 * 1024
        ),
        name="halo",
    )(*arguments)
    outs = [face, face, taller, face]
    trace_x, trace_y, trace_z, pressure = pl.pallas_call(
        combine_kernel,
        out_shape=[jax.ShapeDtypeStruct(shape, F32) for shape in outs],
        in_specs=[pl.BlockSpec(memory_space=pltpu.VMEM)] * len(shapes),
        out_specs=[pl.BlockSpec(memory_space=pl.ANY)] * 4,
        scratch_shapes=[pltpu.VMEM(shape, F32) for shape in outs]
        + [pltpu.SemaphoreType.DMA((5, 4))],
        compiler_params=pltpu.CompilerParams(vmem_limit_bytes=20 * 1024 * 1024),
        name="combine",
    )(*held)
    trace_z = jnp.transpose(trace_z.reshape(levels + 1, n, m), (1, 0, 2))
    return trace_x, trace_y, trace_z, pressure


def solution(mesh):
    px, py = mesh.shape["px"], mesh.shape["py"]
    columns = P("px", None, "py")
    return jax.shard_map(
        functools.partial(local, px, py),
        mesh=mesh,
        in_specs=(P(None, "px", None, "py"), columns, columns, P("px", "py"), columns, columns, columns),
        out_specs=(columns,) * 4,
        check_vma=False,
    )
```

```python
import functools
import itertools

import jax
import jax.numpy as jnp
from jax import lax
from jax.experimental import pallas as pl
from jax.experimental.pallas import tpu as pltpu
from jax.sharding import PartitionSpec as P

MESH = pl.DeviceIdType.MESH
F32 = jnp.float32
SPARE = 100


def factors(px, py):
    if px == 16 and py == 32:
        return (2, 4, 2), (4, 8)
    return (1, px // 2, 2), (2, py // 2)


def peers(px, py, me_x, me_y, dims):
    (ny_lo, nx, nc), (ny_hi, nz) = factors(px, py)
    sizes = {"y_lo": ny_lo, "x": nx, "core": nc, "y_hi": ny_hi, "z": nz}
    here = {
        "core": lax.rem(me_x, nc),
        "x": lax.rem(me_x // nc, nx),
        "y_lo": me_x // (nc * nx),
        "z": lax.rem(me_y, nz),
        "y_hi": me_y // nz,
    }
    reach = {"core": 0, "x": 1, "y_lo": 1, "z": 1, "y_hi": 2}

    def far(offset):
        return sum(reach[d] * min(o, sizes[d] - o) for d, o in zip(dims, offset))

    found = []
    offsets = itertools.product(*[range(sizes[d]) for d in dims])
    for offset in sorted(offsets, key=far, reverse=True):
        if not any(offset):
            continue
        there = dict(here)
        for d, o in zip(dims, offset):
            there[d] = lax.rem(here[d] + o, sizes[d])
        found.append(
            {
                "px": (there["y_lo"] * nx + there["x"]) * nc + there["core"],
                "py": there["y_hi"] * nz + there["z"],
            }
        )
    return found


PHASES = (("core", "z"), ("x", "y_lo", "y_hi"))


def group_size(px, py, dims):
    (ny_lo, nx, nc), (ny_hi, nz) = factors(px, py)
    sizes = {"y_lo": ny_lo, "x": nx, "core": nc, "y_hi": ny_hi, "z": nz}
    total = 1
    for d in dims:
        total *= sizes[d]
    return total


def cell(w, e, s, n, b, t, ix, iy, iz, rd, g):
    sx, sy, sz = w + e, s + n, b + t
    total = 3.0 * (ix * sx + iy * sy + iz * sz)
    if g is not None:
        total = total + g
    p = total * rd
    p3 = 3.0 * p
    qx, qy, qz = sx - p3, sy - p3, sz - p3
    return (
        (ix * (qx + w), ix * (qx + e), iy * (qy + s), iy * (qy + n), iz * (qz + b), iz * (qz + t)),
        p,
    )


def halo_kernel(
    px, py,
    metric_h, helm_h, forc_h, orient_h, sx_h, sy_h, sz_h,
    x_ref, y_ref, z_ref, rx, ry, rz, wx, wy, wz, p0, p1, p2, coef,
    metric, helm, forc, orient, ix_s, iy_s, iz_s, rd_s,
    z_x, rz_x, wz_x, tb, send_b, recv_b, msg_s, msg_r, str_s, str_r, dia_s, dia_r, row_b, *rest,
):
    slots = rest[: len(PHASES)]
    load_sem, send_sem, recv_sem, ar_send, ar_recv = rest[len(PHASES) :]
    n, levels, m = helm.shape
    me_x, me_y = lax.axis_index("px"), lax.axis_index("py")
    west = {"px": lax.rem(me_x + px - 1, px), "py": me_y}
    east = {"px": lax.rem(me_x + 1, px), "py": me_y}
    south = {"px": me_x, "py": lax.rem(me_y + py - 1, py)}
    north = {"px": me_x, "py": lax.rem(me_y + 1, py)}
    corner = [
        {"px": x["px"], "py": y["py"]} for x in (east, west) for y in (north, south)
    ]
    groups = [peers(px, py, me_x, me_y, dims) for dims in PHASES]

    loads = [
        pltpu.make_async_copy(src, dst, load_sem.at[k])
        for k, (src, dst) in enumerate(
            [
                (sy_h, y_ref),
                (sx_h, x_ref.at[pl.ds(0, n)]),
                (metric_h, metric),
                (orient_h, orient),
                (helm_h, helm),
                (forc_h, forc),
                (sz_h, z_ref),
            ]
        )
    ]
    for load in loads:
        load.start()

    barrier = pltpu.get_barrier_semaphore()
    greeted = [west, east, south, north] + corner + [d for group in groups for d in group]
    for device in greeted:
        pl.semaphore_signal(barrier, inc=1, device_id=device, device_id_type=MESH)

    lane = lax.broadcasted_iota(jnp.int32, (levels, m), 1)
    level = lax.broadcasted_iota(jnp.int32, (levels, m), 0)
    pair = jnp.right_shift(lane, 1)
    odd = jnp.bitwise_and(lane, 1) == 1
    zero = jnp.zeros((levels, m), F32)

    def into_strip(i, value, strip):
        return jnp.where(pair == i, pltpu.roll(value, 2 * i + 1, 1), strip)

    def lane1_into_strip(i, value, strip):
        return jnp.where(lane == 2 * i + 1, pltpu.roll(value, 2 * i, 1), strip)

    def exchange(source, target, slot, device):
        return pltpu.make_async_remote_copy(
            src_ref=source,
            dst_ref=target,
            send_sem=send_sem.at[slot],
            recv_sem=recv_sem.at[slot],
            device_id=device,
            device_id_type=MESH,
        )

    for load in loads:
        load.wait()

    def coefficient(i, strips):
        a = 1.0 / metric[0, i].astype(F32)
        b = 1.0 / metric[1, i].astype(F32)
        c = 1.0 / metric[2, i].astype(F32)
        turned = orient[pl.ds(i, 1), :] == 1
        values = (
            jnp.where(turned, b, a),
            jnp.where(turned, a, b),
            c,
            1.0 / (helm[i].astype(F32) + 6.0 * (a + b + c)),
            forc[i].astype(F32),
        )
        ix_s[i], iy_s[i], iz_s[i], rd_s[i], _ = values
        return tuple(into_strip(i, v, strip) for v, strip in zip(values, strips))

    strips = lax.fori_loop(0, n, coefficient, (zero,) * 5, unroll=8)
    for k in range(5):
        tb[k] = strips[k]

    def vertical(i, ref):
        return ref[i, pl.ds(0, levels), :], ref[i, pl.ds(1, levels), :]

    def collect(fields, base):
        fx, fy, fz = fields

        def body(i, strips):
            y = fy[i]
            b, t = vertical(i, fz)
            return (
                into_strip(i, fx[i], strips[0]),
                into_strip(i, y, strips[1]),
                lane1_into_strip(i, y, strips[2]),
                into_strip(i, b, strips[3]),
                into_strip(i, t, strips[4]),
            )

        strips = lax.fori_loop(0, n, body, (zero,) * 5, unroll=8)
        for k in range(5):
            tb[base + k] = strips[k]

    def row(i, fields, strip, fresh, source):
        fx, fy, fz = fields
        edge = pltpu.roll(strip, m - 1 - 2 * i, 1)
        s = fy[i]
        if not fresh:
            s = s + jnp.where(lane == 0, edge, 0.0)
        north_side = jnp.where(lane == m - 1, edge, pltpu.roll(s, m - 1, 1))
        b, t = vertical(i, fz)
        w, e = fx[i], fx[i + 1]
        g = forc[i].astype(F32) if source else None
        flux, p = cell(w, e, s, north_side, b, t, ix_s[i], iy_s[i], iz_s[i], rd_s[i], g)
        return (w, e, s, north_side, b, t), flux, p

    def strip_flux(base, last, strip, source):
        te = jnp.where(pair == n - 1, pltpu.roll(last, 2 * n - 1, 1), pltpu.roll(tb[base], m - 2, 1))
        tn = jnp.where(odd, tb[base + 2], strip)
        return cell(
            tb[base], te, tb[base + 1], tn, tb[base + 3], tb[base + 4],
            tb[0], tb[1], tb[2], tb[3], tb[4] if source else None,
        )[0]

    def assemble(i, flux, fe_before, outs, sign):
        fw, fe, fs, fn, fb, ft = flux
        out_x, out_y, out_z = outs
        out_x[i] = sign * (fw + fe_before)
        out_y[i] = sign * (fs + jnp.where(lane == 0, 0.0, pltpu.roll(fn, 1, 1)))
        shifted = pltpu.roll(ft, 1, 0)
        out_z[i, pl.ds(0, levels), :] = sign * (fb + jnp.where(level == 0, 0.0, shifted))
        out_z[i, pl.ds(levels, 1), :] = sign * shifted[0:1]
        return fe

    start = (x_ref, y_ref, z_x)
    residual = (rx, ry, rz_x)
    image = (wx, wy, wz_x)

    def turn(i, carry):
        z_x[i] = z_ref[pl.ds(i, levels + 1, stride=n), :]
        return carry

    lax.fori_loop(0, n, turn, 0, unroll=4)
    x_ref[n] = zero
    collect(start, 5)

    flux = strip_flux(5, zero, zero, True)
    both = 9.0 * tb[0] * tb[1] * tb[3]
    spare = lane == SPARE
    slab = jnp.where(odd, tb[6], pltpu.roll(-flux[2], m - 1, 1))
    str_s[0] = jnp.where(spare, pltpu.roll(both, (SPARE - 2 * n + 1) % m, 1), slab)
    slope = 9.0 * tb[1] * tb[1] * tb[3] - 2.0 * tb[1]
    slab = jnp.where(odd, pltpu.roll(slope, 1, 1), -flux[3])
    str_s[1] = jnp.where(spare, pltpu.roll(both, (SPARE - 2 * n + 2) % m, 1), slab)
    msg_s[0, 0] = x_ref[0]
    msg_s[0, 1] = -row(0, start, zero, True, True)[1][0]
    msg_s[0, 2] = 9.0 * ix_s[0] * iy_s[0] * rd_s[0]
    msg_s[1, 0] = -row(n - 1, start, zero, True, True)[1][1]
    msg_s[1, 1] = 9.0 * ix_s[n - 1] * ix_s[n - 1] * rd_s[n - 1] - 2.0 * ix_s[n - 1]
    msg_s[1, 2] = 9.0 * ix_s[n - 1] * iy_s[n - 1] * rd_s[n - 1]
    dia_s[0] = jnp.where(
        lane == m - 1, pltpu.roll(y_ref[0], m - 1, 1), pltpu.roll(x_ref[0], 2 * n - 1, 1)
    )
    dia_s[1] = pltpu.roll(y_ref[n - 1], m - 1, 1)
    north_east, south_east, north_west, south_west = corner
    first = [
        exchange(dia_s.at[0], dia_r.at[0], 8, south_west),
        exchange(dia_s.at[0], dia_r.at[1], 9, north_west),
        exchange(dia_s.at[1], dia_r.at[2], 10, south_east),
    ] + [
        exchange(str_s.at[0], str_r.at[0], 6, south),
        exchange(str_s.at[1], str_r.at[1], 7, north),
        exchange(msg_s.at[0], msg_r.at[0], 4, west),
        exchange(msg_s.at[1], msg_r.at[1], 5, east),
    ]
    pl.semaphore_wait(barrier, len(greeted))
    for copy in first:
        copy.start()

    def pass1(i, fe_before):
        _, flux, _ = row(i, start, zero, True, True)
        return assemble(i, flux, fe_before, residual, -1.0)

    lax.fori_loop(0, n, pass1, zero, unroll=8)
    collect(residual, 11)

    for copy in first:
        copy.wait_recv()
    x_ref[n] = msg_r[0, 0]
    north_slab, south_slab = str_r[0], str_r[1]
    strip1 = pltpu.roll(north_slab, m - 1, 1)
    from_east = msg_r[0, 1] + jnp.where(lane == m - 1, msg_r[0, 2] * dia_r[0], 0.0)
    from_west = (
        msg_r[1, 0]
        + msg_r[1, 1] * x_ref[0]
        + jnp.where(lane == m - 1, msg_r[1, 2] * dia_r[2], 0.0)
    )
    both = pltpu.roll(north_slab, (2 * n - 1 - SPARE) % m, 1)
    from_north = pltpu.roll(north_slab, 1, 1) + jnp.where(lane == 2 * n - 1, both * dia_r[0], 0.0)
    both = pltpu.roll(south_slab, (2 * n - 2 - SPARE) % m, 1)
    from_south = (
        south_slab
        + pltpu.roll(south_slab, m - 1, 1) * pltpu.roll(tb[6], m - 1, 1)
        + jnp.where(lane == 2 * n - 2, both * dia_r[1], 0.0)
    )
    high = pltpu.roll(from_north, m - 1, 1) - strip_flux(5, x_ref[n], strip1, True)[3]
    strip2 = jnp.where(odd, pltpu.roll(from_south, 1, 1), high)

    own = jnp.where(odd, 0.0, strip1)
    dp = 3.0 * tb[1] * tb[3] * own
    dx, dz = 3.0 * tb[0] * dp, 3.0 * tb[2] * dp
    add_x = dx + pltpu.roll(dx, 2, 1)
    add_y = 3.0 * tb[1] * dp - tb[1] * own
    add_b = dz + jnp.where(level == 0, 0.0, pltpu.roll(dz, 1, 0))
    add_t = dz + jnp.where(level == levels - 1, 0.0, pltpu.roll(dz, levels - 1, 0))

    f0 = row(0, start, strip1, True, True)[1]
    assemble(0, f0, -from_west, residual, -1.0)
    assemble(1, row(1, start, strip1, True, True)[1], f0[1], residual, -1.0)
    before = row(n - 2, start, strip1, True, True)[1][1]
    fe_last = assemble(n - 1, row(n - 1, start, strip1, True, True)[1], before, residual, -1.0)
    rx[n] = from_east - fe_last
    b_last, t_last = vertical(n - 1, rz_x)
    tb[11] = into_strip(0, rx[0], into_strip(n - 1, rx[n - 1], tb[11] + add_x))
    tb[12] = into_strip(n - 1, ry[n - 1], tb[12] + add_y) + jnp.where(odd, strip2, 0.0)
    tb[13] = lane1_into_strip(n - 1, ry[n - 1], tb[13])
    tb[14] = into_strip(n - 1, b_last, tb[14] + add_b)
    tb[15] = into_strip(n - 1, t_last, tb[15] + add_t)

    flux = strip_flux(11, rx[n], strip2, False)
    send_b[2] = jnp.where(odd, flux[2], flux[3])
    send_b[0] = row(0, residual, strip2, False, False)[1][0]
    send_b[1] = row(n - 1, residual, strip2, False, False)[1][1]
    second = [
        exchange(send_b.at[2], recv_b.at[2], 2, south),
        exchange(send_b.at[2], recv_b.at[3], 3, north),
        exchange(send_b.at[0], recv_b.at[0], 0, west),
        exchange(send_b.at[1], recv_b.at[1], 1, east),
    ]
    for copy in second:
        copy.start()

    rows_left = jnp.logical_and(pair > 1, pair < n - 1)
    adds = [jnp.where(rows_left, a, 0.0) for a in (add_x, add_y, add_b, add_t)]

    def amend(i, carry):
        ax, ay, ab, at = [
            jnp.where(lane == m - 1, pltpu.roll(a, m - 1 - 2 * i, 1), 0.0) for a in adds
        ]
        rx[i] = rx[i] + ax
        ry[i] = ry[i] + ay
        rz_x[i, pl.ds(0, levels), :] = rz_x[i, pl.ds(0, levels), :] + ab
        top = pl.ds(levels, 1)
        rz_x[i, top, :] = rz_x[i, top, :] + at[levels - 1 :]
        return carry

    lax.fori_loop(0, n, amend, 0, unroll=8)

    def pass2(i, carry):
        fe_before, rr = carry
        (w, e, s, north_side, b, t), flux, p = row(i, residual, strip2, False, False)
        ry[i] = s
        p1[i] = p
        top = jnp.where(level == levels - 1, t, 0.0)
        rr = rr + (w * w + s * s + b * b + top * top)
        return assemble(i, flux, fe_before, image, 1.0), rr

    wx[n], rr = lax.fori_loop(0, n, pass2, (zero, zero), unroll=8)

    collect(image, 5)

    inner = jnp.logical_and(lane > 0, lane < m - 1)

    def quadratic(faces, flux):
        w, e, s, north_side, b, t = faces
        fw, fe, fs, fn, fb, ft = flux
        return (w * fw + e * fe) + (s * fs + north_side * fn) + (b * fb + t * ft)

    def pass3(i, carry):
        rw, ww, waw = carry
        s = wy[i]
        north_side = pltpu.roll(s, m - 1, 1)
        b, t = vertical(i, wz_x)
        rb, rt = vertical(i, rz_x)
        w, e = wx[i], wx[i + 1]
        flux, _ = cell(w, e, s, north_side, b, t, ix_s[i], iy_s[i], iz_s[i], rd_s[i], None)
        between = jnp.logical_and(i > 0, i < n - 1)
        sm = jnp.where(lane == 0, 0.0, s)
        top = jnp.where(level == levels - 1, t, 0.0)
        rw = rw + jnp.where(between, w * rx[i] + sm * ry[i] + b * rb + top * rt, 0.0)
        ww = ww + jnp.where(between, w * w + sm * sm + b * b + top * top, 0.0)
        kept = jnp.logical_and(inner, between)
        waw = waw + jnp.where(kept, quadratic((w, e, s, north_side, b, t), flux), 0.0)
        return rw, ww, waw

    rw, ww, waw = lax.fori_loop(0, n, pass3, (zero, zero, zero), unroll=8)

    for copy in second:
        copy.wait_recv()
    wx[0] = wx[0] + recv_b[1]
    wx[n] = wx[n] + recv_b[0]
    high = send_b[2] + pltpu.roll(recv_b[2], m - 1, 1)
    strip3 = jnp.where(odd, pltpu.roll(recv_b[3], 1, 1), high)
    rest_of = jnp.logical_and(pair > 0, pair < n - 1)
    tw, ts = tb[5], tb[6] + jnp.where(odd, strip3, 0.0)
    te, tn = pltpu.roll(tw, m - 2, 1), jnp.where(odd, tb[7], strip3)
    faces = (tw, te, ts, tn, tb[8], tb[9])
    flux, _ = cell(*faces, tb[0], tb[1], tb[2], tb[3], None)
    waw = waw + jnp.where(rest_of, quadratic(faces, flux), 0.0)
    ts = jnp.where(jnp.logical_and(rest_of, odd), ts, 0.0)
    ww = ww + ts * ts
    rw = rw + ts * tb[12]
    for i in (0, n - 1):
        faces, flux, _ = row(i, image, strip3, False, False)
        w, _, s, _, b, t = faces
        rb, rt = vertical(i, rz_x)
        top = jnp.where(level == levels - 1, t, 0.0)
        rw = rw + (w * rx[i] + s * ry[i] + b * rb + top * rt)
        ww = ww + (w * w + s * s + b * b + top * top)
        waw = waw + quadratic(faces, flux)

    def finish(i, carry):
        faces, _, p = row(i, image, strip3, False, False)
        wy[i] = faces[2]
        p2[i] = p
        p0[i] = row(i, start, strip1, True, True)[2]
        rz[pl.ds(i, levels + 1, stride=n), :] = rz_x[i]
        wz[pl.ds(i, levels + 1, stride=n), :] = wz_x[i]
        return carry

    lane_row = lax.broadcasted_iota(jnp.int32, (1, m), 1)
    sums = jnp.zeros((1, m), F32)
    for k, part in enumerate((rr, rw, ww, waw)):
        whole = jnp.sum(jnp.sum(part, axis=0, keepdims=True), axis=1, keepdims=True)
        sums = jnp.where(lane_row == k, whole, sums)

    for k, (group, slot) in enumerate(zip(groups, slots)):
        row_b[k] = sums
        for j, device in enumerate(group):
            pltpu.make_async_remote_copy(
                src_ref=row_b.at[pl.ds(k, 1)],
                dst_ref=slot.at[pl.ds(j, 1)],
                send_sem=ar_send.at[k],
                recv_sem=ar_recv.at[k],
                device_id=device,
                device_id_type=MESH,
            ).start()
        if k == 0:
            lax.fori_loop(0, n, finish, 0, unroll=4)
        everything = pltpu.make_async_remote_copy(
            src_ref=slot, dst_ref=slot, send_sem=ar_send.at[k], recv_sem=ar_recv.at[k],
            device_id=group[0], device_id_type=MESH,
        )
        everything.wait_recv()
        sums = sums + jnp.sum(slot[...], axis=0)
        everything.wait_send()

    rr, rw, ww, waw = [
        jnp.sum(jnp.where(lane_row == k, sums, 0.0), axis=1, keepdims=True) for k in range(4)
    ]
    a0 = rr / rw
    grown = ww * a0 / rw
    b = grown - 1.0
    a1 = b * rr / (a0 * a0 * waw - grown * grown * rw)
    coef[0] = jnp.broadcast_to(a0 + a1 * grown, coef.shape[1:])
    coef[1] = jnp.broadcast_to(-a1 * a0, coef.shape[1:])
    for copy in first + second:
        copy.wait_send()


def combine_kernel(
    x_ref, y_ref, z_ref, rx, ry, rz, wx, wy, wz, p0, p1, p2, coef,
    ox_h, oy_h, oz_h, op_h, ox, oy, oz, op, sem,
):
    n = ox.shape[0]
    chunks = 5
    rows = n // chunks
    step = n
    c1, c2 = coef[0, 0:1, :], coef[1, 0:1, :]
    copies = []
    for k in range(chunks):

        def body(i, carry):
            ox[i] = x_ref[i] + (c1 * rx[i] + c2 * wx[i])
            oy[i] = y_ref[i] + (c1 * ry[i] + c2 * wy[i])
            op[i] = p0[i] + (c1 * p1[i] + c2 * p2[i])
            return carry

        lax.fori_loop(k * rows, (k + 1) * rows, body, 0)
        tall = oz.shape[0] // chunks

        def body_z(i, carry):
            at = pl.ds(pl.multiple_of(i * step, step), step)
            oz[at, :] = z_ref[at, :] + (c1 * rz[at, :] + c2 * wz[at, :])
            return carry

        lax.fori_loop(k * (tall // step), (k + 1) * (tall // step), body_z, 0)
        span = pl.ds(k * rows, rows)
        span_z = pl.ds(k * tall, tall)
        for j, (src, dst, at) in enumerate(
            ((ox, ox_h, span), (oy, oy_h, span), (oz, oz_h, span_z), (op, op_h, span))
        ):
            copy = pltpu.make_async_copy(src.at[at], dst.at[at], sem.at[k, j])
            copy.start()
            copies.append(copy)
    for copy in copies:
        copy.wait()


def local(px, py, metric, helmholtz, forcing, orientation, start_x, start_y, start_z):
    n, levels, m = helmholtz.shape
    face = (n, levels, m)
    longer = (n + 1, levels, m)
    taller = ((levels + 1) * n, m)
    start_z = jnp.transpose(start_z, (1, 0, 2)).reshape(taller)
    arguments = [
        pltpu.with_memory_space_constraint(a, pltpu.HBM)
        for a in (metric, helmholtz, forcing, orientation, start_x, start_y, start_z)
    ]
    shapes = [longer, face, taller, longer, face, taller, longer, face, taller, face, face, face, (2, 8, m)]
    held = pl.pallas_call(
        functools.partial(halo_kernel, px, py),
        out_shape=[pltpu.VMEM(shape, F32) for shape in shapes],
        in_specs=[pl.BlockSpec(memory_space=pl.ANY)] * 7,
        out_specs=[pl.BlockSpec(memory_space=pltpu.VMEM)] * len(shapes),
        scratch_shapes=[
            pltpu.VMEM((3,) + face, metric.dtype),
            pltpu.VMEM(face, helmholtz.dtype),
            pltpu.VMEM(face, forcing.dtype),
            pltpu.VMEM((n, m), jnp.int32),
            pltpu.VMEM(face, F32),
            pltpu.VMEM(face, F32),
            pltpu.VMEM(face, F32),
            pltpu.VMEM(face, F32),
            pltpu.VMEM((n, levels + 1, m), F32),
            pltpu.VMEM((n, levels + 1, m), F32),
            pltpu.VMEM((n, levels + 1, m), F32),
            pltpu.VMEM((16, levels, m), F32),
            pltpu.VMEM((3, levels, m), F32),
            pltpu.VMEM((4, levels, m), F32),
            pltpu.VMEM((2, 3, levels, m), F32),
            pltpu.VMEM((2, 3, levels, m), F32),
            pltpu.VMEM((2, levels, m), F32),
            pltpu.VMEM((2, levels, m), F32),
            pltpu.VMEM((2, levels, m), F32),
            pltpu.VMEM((3, levels, m), F32),
            pltpu.VMEM((len(PHASES), 1, m), F32),
        ]
        + [pltpu.VMEM((group_size(px, py, dims) - 1, 1, m), F32) for dims in PHASES]
        + [
            pltpu.SemaphoreType.DMA((7,)),
            pltpu.SemaphoreType.DMA((11,)),
            pltpu.SemaphoreType.DMA((11,)),
            pltpu.SemaphoreType.DMA((len(PHASES),)),
            pltpu.SemaphoreType.DMA((len(PHASES),)),
        ],
        compiler_params=pltpu.CompilerParams(
            collective_id=0, has_side_effects=True, vmem_limit_bytes=40 * 1024 * 1024
        ),
        name="halo",
    )(*arguments)
    outs = [face, face, taller, face]
    trace_x, trace_y, trace_z, pressure = pl.pallas_call(
        combine_kernel,
        out_shape=[jax.ShapeDtypeStruct(shape, F32) for shape in outs],
        in_specs=[pl.BlockSpec(memory_space=pltpu.VMEM)] * len(shapes),
        out_specs=[pl.BlockSpec(memory_space=pl.ANY)] * 4,
        scratch_shapes=[pltpu.VMEM(shape, F32) for shape in outs]
        + [pltpu.SemaphoreType.DMA((5, 4))],
        compiler_params=pltpu.CompilerParams(vmem_limit_bytes=20 * 1024 * 1024),
        name="combine",
    )(*held)
    trace_z = jnp.transpose(trace_z.reshape(levels + 1, n, m), (1, 0, 2))
    return trace_x, trace_y, trace_z, pressure


def solution(mesh):
    px, py = mesh.shape["px"], mesh.shape["py"]
    columns = P("px", None, "py")
    return jax.shard_map(
        functools.partial(local, px, py),
        mesh=mesh,
        in_specs=(P(None, "px", None, "py"), columns, columns, P("px", "py"), columns, columns, columns),
        out_specs=(columns,) * 4,
        check_vma=False,
    )
```

```python
import functools
import itertools

import jax
import jax.numpy as jnp
from jax import lax
from jax.experimental import pallas as pl
from jax.experimental.pallas import tpu as pltpu
from jax.sharding import PartitionSpec as P

MESH = pl.DeviceIdType.MESH
F32 = jnp.float32
SPARE = 100


def factors(px, py):
    if px == 16 and py == 32:
        return (2, 4, 2), (4, 8)
    return (1, px // 2, 2), (2, py // 2)


def peers(px, py, me_x, me_y, dims):
    (ny_lo, nx, nc), (ny_hi, nz) = factors(px, py)
    sizes = {"y_lo": ny_lo, "x": nx, "core": nc, "y_hi": ny_hi, "z": nz}
    here = {
        "core": lax.rem(me_x, nc),
        "x": lax.rem(me_x // nc, nx),
        "y_lo": me_x // (nc * nx),
        "z": lax.rem(me_y, nz),
        "y_hi": me_y // nz,
    }
    reach = {"core": 0, "x": 1, "y_lo": 1, "z": 1, "y_hi": 2}

    def far(offset):
        return sum(reach[d] * min(o, sizes[d] - o) for d, o in zip(dims, offset))

    found = []
    offsets = itertools.product(*[range(sizes[d]) for d in dims])
    for offset in sorted(offsets, key=far, reverse=True):
        if not any(offset):
            continue
        there = dict(here)
        for d, o in zip(dims, offset):
            there[d] = lax.rem(here[d] + o, sizes[d])
        found.append(
            {
                "px": (there["y_lo"] * nx + there["x"]) * nc + there["core"],
                "py": there["y_hi"] * nz + there["z"],
            }
        )
    return found


PHASES = (("core", "z"), ("x", "y_lo", "y_hi"))


def group_size(px, py, dims):
    (ny_lo, nx, nc), (ny_hi, nz) = factors(px, py)
    sizes = {"y_lo": ny_lo, "x": nx, "core": nc, "y_hi": ny_hi, "z": nz}
    total = 1
    for d in dims:
        total *= sizes[d]
    return total


def cell(w, e, s, n, b, t, ix, iy, iz, rd, g):
    sx, sy, sz = w + e, s + n, b + t
    total = 3.0 * (ix * sx + iy * sy + iz * sz)
    if g is not None:
        total = total + g
    p = total * rd
    p3 = 3.0 * p
    qx, qy, qz = sx - p3, sy - p3, sz - p3
    return (
        (ix * (qx + w), ix * (qx + e), iy * (qy + s), iy * (qy + n), iz * (qz + b), iz * (qz + t)),
        p,
    )


def halo_kernel(
    px, py,
    metric_h, helm_h, forc_h, orient_h, sx_h, sy_h, sz_h,
    x_ref, y_ref, z_ref, rx, ry, rz, wx, wy, wz, p0, p1, p2, coef,
    metric, helm, forc, orient, ix_s, iy_s, iz_s, rd_s,
    z_x, rz_x, wz_x, tb, send_b, recv_b, msg_s, msg_r, str_s, str_r, dia_s, dia_r, row_b, *rest,
):
    slots = rest[: len(PHASES)]
    load_sem, send_sem, recv_sem, ar_send, ar_recv = rest[len(PHASES) :]
    n, levels, m = helm.shape
    me_x, me_y = lax.axis_index("px"), lax.axis_index("py")
    west = {"px": lax.rem(me_x + px - 1, px), "py": me_y}
    east = {"px": lax.rem(me_x + 1, px), "py": me_y}
    south = {"px": me_x, "py": lax.rem(me_y + py - 1, py)}
    north = {"px": me_x, "py": lax.rem(me_y + 1, py)}
    corner = [
        {"px": x["px"], "py": y["py"]} for x in (east, west) for y in (north, south)
    ]
    groups = [peers(px, py, me_x, me_y, dims) for dims in PHASES]

    loads = [
        pltpu.make_async_copy(src, dst, load_sem.at[k])
        for k, (src, dst) in enumerate(
            [
                (sy_h, y_ref),
                (sx_h, x_ref.at[pl.ds(0, n)]),
                (metric_h, metric),
                (orient_h, orient),
                (helm_h, helm),
                (forc_h, forc),
                (sz_h, z_ref),
            ]
        )
    ]
    for load in loads:
        load.start()

    barrier = pltpu.get_barrier_semaphore()
    greeted = [west, east, south, north] + corner + [d for group in groups for d in group]
    for device in greeted:
        pl.semaphore_signal(barrier, inc=1, device_id=device, device_id_type=MESH)

    lane = lax.broadcasted_iota(jnp.int32, (levels, m), 1)
    level = lax.broadcasted_iota(jnp.int32, (levels, m), 0)
    pair = jnp.right_shift(lane, 1)
    odd = jnp.bitwise_and(lane, 1) == 1
    zero = jnp.zeros((levels, m), F32)

    def into_strip(i, value, strip):
        return jnp.where(pair == i, pltpu.roll(value, 2 * i + 1, 1), strip)

    def lane1_into_strip(i, value, strip):
        return jnp.where(lane == 2 * i + 1, pltpu.roll(value, 2 * i, 1), strip)

    def exchange(source, target, slot, device):
        return pltpu.make_async_remote_copy(
            src_ref=source,
            dst_ref=target,
            send_sem=send_sem.at[slot],
            recv_sem=recv_sem.at[slot],
            device_id=device,
            device_id_type=MESH,
        )

    for load in loads:
        load.wait()

    def coefficient(i, strips):
        a = 1.0 / metric[0, i].astype(F32)
        b = 1.0 / metric[1, i].astype(F32)
        c = 1.0 / metric[2, i].astype(F32)
        turned = orient[pl.ds(i, 1), :] == 1
        values = (
            jnp.where(turned, b, a),
            jnp.where(turned, a, b),
            c,
            1.0 / (helm[i].astype(F32) + 6.0 * (a + b + c)),
            forc[i].astype(F32),
        )
        ix_s[i], iy_s[i], iz_s[i], rd_s[i], _ = values
        return tuple(into_strip(i, v, strip) for v, strip in zip(values, strips))

    strips = lax.fori_loop(0, n, coefficient, (zero,) * 5, unroll=8)
    for k in range(5):
        tb[k] = strips[k]

    def vertical(i, ref):
        return ref[i, pl.ds(0, levels), :], ref[i, pl.ds(1, levels), :]

    def collect(fields, base):
        fx, fy, fz = fields

        def body(i, strips):
            y = fy[i]
            b, t = vertical(i, fz)
            return (
                into_strip(i, fx[i], strips[0]),
                into_strip(i, y, strips[1]),
                lane1_into_strip(i, y, strips[2]),
                into_strip(i, b, strips[3]),
                into_strip(i, t, strips[4]),
            )

        strips = lax.fori_loop(0, n, body, (zero,) * 5, unroll=8)
        for k in range(5):
            tb[base + k] = strips[k]

    def row(i, fields, strip, fresh, source):
        fx, fy, fz = fields
        edge = pltpu.roll(strip, m - 1 - 2 * i, 1)
        s = fy[i]
        if not fresh:
            s = s + jnp.where(lane == 0, edge, 0.0)
        north_side = jnp.where(lane == m - 1, edge, pltpu.roll(s, m - 1, 1))
        b, t = vertical(i, fz)
        w, e = fx[i], fx[i + 1]
        g = forc[i].astype(F32) if source else None
        flux, p = cell(w, e, s, north_side, b, t, ix_s[i], iy_s[i], iz_s[i], rd_s[i], g)
        return (w, e, s, north_side, b, t), flux, p

    def strip_flux(base, last, strip, source):
        te = jnp.where(pair == n - 1, pltpu.roll(last, 2 * n - 1, 1), pltpu.roll(tb[base], m - 2, 1))
        tn = jnp.where(odd, tb[base + 2], strip)
        return cell(
            tb[base], te, tb[base + 1], tn, tb[base + 3], tb[base + 4],
            tb[0], tb[1], tb[2], tb[3], tb[4] if source else None,
        )[0]

    def assemble(i, flux, fe_before, outs, sign):
        fw, fe, fs, fn, fb, ft = flux
        out_x, out_y, out_z = outs
        out_x[i] = sign * (fw + fe_before)
        out_y[i] = sign * (fs + jnp.where(lane == 0, 0.0, pltpu.roll(fn, 1, 1)))
        shifted = pltpu.roll(ft, 1, 0)
        out_z[i, pl.ds(0, levels), :] = sign * (fb + jnp.where(level == 0, 0.0, shifted))
        out_z[i, pl.ds(levels, 1), :] = sign * shifted[0:1]
        return fe

    start = (x_ref, y_ref, z_x)
    residual = (rx, ry, rz_x)
    image = (wx, wy, wz_x)

    def turn(i, carry):
        z_x[i] = z_ref[pl.ds(i, levels + 1, stride=n), :]
        return carry

    lax.fori_loop(0, n, turn, 0, unroll=4)
    x_ref[n] = zero
    collect(start, 5)

    flux = strip_flux(5, zero, zero, True)
    both = 9.0 * tb[0] * tb[1] * tb[3]
    spare = lane == SPARE
    slab = jnp.where(odd, tb[6], pltpu.roll(-flux[2], m - 1, 1))
    str_s[0] = jnp.where(spare, pltpu.roll(both, (SPARE - 2 * n + 1) % m, 1), slab)
    slope = 9.0 * tb[1] * tb[1] * tb[3] - 2.0 * tb[1]
    slab = jnp.where(odd, pltpu.roll(slope, 1, 1), -flux[3])
    str_s[1] = jnp.where(spare, pltpu.roll(both, (SPARE - 2 * n + 2) % m, 1), slab)
    msg_s[0, 0] = x_ref[0]
    msg_s[0, 1] = -row(0, start, zero, True, True)[1][0]
    msg_s[0, 2] = 9.0 * ix_s[0] * iy_s[0] * rd_s[0]
    msg_s[1, 0] = -row(n - 1, start, zero, True, True)[1][1]
    msg_s[1, 1] = 9.0 * ix_s[n - 1] * ix_s[n - 1] * rd_s[n - 1] - 2.0 * ix_s[n - 1]
    msg_s[1, 2] = 9.0 * ix_s[n - 1] * iy_s[n - 1] * rd_s[n - 1]
    def as_row(columns):
        spread = zero
        for k, column in enumerate(columns):
            spread = jnp.where(lane == level + 32 * k, column, spread)
        return jnp.sum(spread, axis=0, keepdims=True)

    def as_column(line, k):
        return jnp.sum(jnp.where(lane == level + 32 * k, line, 0.0), axis=1, keepdims=True)

    y_first, x_first, y_last = y_ref[0][:, 0:1], x_ref[0], y_ref[n - 1][:, 0:1]
    dia_s[0] = as_row((y_first, x_first[:, 0:1], x_first[:, m - 1 :]))
    dia_s[1] = as_row((y_last,))
    north_east, south_east, north_west, south_west = corner
    first = [
        exchange(dia_s.at[0], dia_r.at[0], 8, south_west),
        exchange(dia_s.at[0], dia_r.at[1], 9, north_west),
        exchange(dia_s.at[1], dia_r.at[2], 10, south_east),
    ] + [
        exchange(str_s.at[0], str_r.at[0], 6, south),
        exchange(str_s.at[1], str_r.at[1], 7, north),
        exchange(msg_s.at[0], msg_r.at[0], 4, west),
        exchange(msg_s.at[1], msg_r.at[1], 5, east),
    ]
    pl.semaphore_wait(barrier, len(greeted))
    for copy in first:
        copy.start()

    def pass1(i, fe_before):
        _, flux, _ = row(i, start, zero, True, True)
        return assemble(i, flux, fe_before, residual, -1.0)

    lax.fori_loop(0, n, pass1, zero, unroll=8)
    collect(residual, 11)

    for copy in first:
        copy.wait_recv()
    x_ref[n] = msg_r[0, 0]
    north_east_y, north_east_x = as_column(dia_r[0], 0), as_column(dia_r[0], 1)
    south_east_x, north_west_y = as_column(dia_r[1], 2), as_column(dia_r[2], 0)
    north_slab, south_slab = str_r[0], str_r[1]
    strip1 = pltpu.roll(north_slab, m - 1, 1)
    from_east = msg_r[0, 1] + jnp.where(lane == m - 1, msg_r[0, 2] * north_east_y, 0.0)
    from_west = (
        msg_r[1, 0]
        + msg_r[1, 1] * x_ref[0]
        + jnp.where(lane == m - 1, msg_r[1, 2] * north_west_y, 0.0)
    )
    both = pltpu.roll(north_slab, (2 * n - 1 - SPARE) % m, 1)
    from_north = pltpu.roll(north_slab, 1, 1) + jnp.where(lane == 2 * n - 1, both * north_east_x, 0.0)
    both = pltpu.roll(south_slab, (2 * n - 2 - SPARE) % m, 1)
    from_south = (
        south_slab
        + pltpu.roll(south_slab, m - 1, 1) * pltpu.roll(tb[6], m - 1, 1)
        + jnp.where(lane == 2 * n - 2, both * south_east_x, 0.0)
    )
    high = pltpu.roll(from_north, m - 1, 1) - strip_flux(5, x_ref[n], strip1, True)[3]
    strip2 = jnp.where(odd, pltpu.roll(from_south, 1, 1), high)

    own = jnp.where(odd, 0.0, strip1)
    dp = 3.0 * tb[1] * tb[3] * own
    dx, dz = 3.0 * tb[0] * dp, 3.0 * tb[2] * dp
    add_x = dx + pltpu.roll(dx, 2, 1)
    add_y = 3.0 * tb[1] * dp - tb[1] * own
    add_b = dz + jnp.where(level == 0, 0.0, pltpu.roll(dz, 1, 0))
    add_t = dz + jnp.where(level == levels - 1, 0.0, pltpu.roll(dz, levels - 1, 0))

    f0 = row(0, start, strip1, True, True)[1]
    assemble(0, f0, -from_west, residual, -1.0)
    assemble(1, row(1, start, strip1, True, True)[1], f0[1], residual, -1.0)
    before = row(n - 2, start, strip1, True, True)[1][1]
    fe_last = assemble(n - 1, row(n - 1, start, strip1, True, True)[1], before, residual, -1.0)
    rx[n] = from_east - fe_last
    b_last, t_last = vertical(n - 1, rz_x)
    tb[11] = into_strip(0, rx[0], into_strip(n - 1, rx[n - 1], tb[11] + add_x))
    tb[12] = into_strip(n - 1, ry[n - 1], tb[12] + add_y) + jnp.where(odd, strip2, 0.0)
    tb[13] = lane1_into_strip(n - 1, ry[n - 1], tb[13])
    tb[14] = into_strip(n - 1, b_last, tb[14] + add_b)
    tb[15] = into_strip(n - 1, t_last, tb[15] + add_t)

    flux = strip_flux(11, rx[n], strip2, False)
    send_b[2] = jnp.where(odd, flux[2], flux[3])
    send_b[0] = row(0, residual, strip2, False, False)[1][0]
    send_b[1] = row(n - 1, residual, strip2, False, False)[1][1]
    second = [
        exchange(send_b.at[2], recv_b.at[2], 2, south),
        exchange(send_b.at[2], recv_b.at[3], 3, north),
        exchange(send_b.at[0], recv_b.at[0], 0, west),
        exchange(send_b.at[1], recv_b.at[1], 1, east),
    ]
    for copy in second:
        copy.start()

    rows_left = jnp.logical_and(pair > 1, pair < n - 1)
    adds = [jnp.where(rows_left, a, 0.0) for a in (add_x, add_y, add_b, add_t)]

    def amend(i, carry):
        ax, ay, ab, at = [
            jnp.where(lane == m - 1, pltpu.roll(a, m - 1 - 2 * i, 1), 0.0) for a in adds
        ]
        rx[i] = rx[i] + ax
        ry[i] = ry[i] + ay
        rz_x[i, pl.ds(0, levels), :] = rz_x[i, pl.ds(0, levels), :] + ab
        top = pl.ds(levels, 1)
        rz_x[i, top, :] = rz_x[i, top, :] + at[levels - 1 :]
        return carry

    lax.fori_loop(0, n, amend, 0, unroll=8)

    def pass2(i, carry):
        fe_before, rr = carry
        (w, e, s, north_side, b, t), flux, p = row(i, residual, strip2, False, False)
        ry[i] = s
        p1[i] = p
        top = jnp.where(level == levels - 1, t, 0.0)
        rr = rr + (w * w + s * s + b * b + top * top)
        return assemble(i, flux, fe_before, image, 1.0), rr

    wx[n], rr = lax.fori_loop(0, n, pass2, (zero, zero), unroll=8)

    collect(image, 5)

    inner = jnp.logical_and(lane > 0, lane < m - 1)

    def quadratic(faces, flux):
        w, e, s, north_side, b, t = faces
        fw, fe, fs, fn, fb, ft = flux
        return (w * fw + e * fe) + (s * fs + north_side * fn) + (b * fb + t * ft)

    def pass3(i, carry):
        rw, ww, waw = carry
        s = wy[i]
        north_side = pltpu.roll(s, m - 1, 1)
        b, t = vertical(i, wz_x)
        rb, rt = vertical(i, rz_x)
        w, e = wx[i], wx[i + 1]
        flux, _ = cell(w, e, s, north_side, b, t, ix_s[i], iy_s[i], iz_s[i], rd_s[i], None)
        between = jnp.logical_and(i > 0, i < n - 1)
        sm = jnp.where(lane == 0, 0.0, s)
        top = jnp.where(level == levels - 1, t, 0.0)
        rw = rw + jnp.where(between, w * rx[i] + sm * ry[i] + b * rb + top * rt, 0.0)
        ww = ww + jnp.where(between, w * w + sm * sm + b * b + top * top, 0.0)
        kept = jnp.logical_and(inner, between)
        waw = waw + jnp.where(kept, quadratic((w, e, s, north_side, b, t), flux), 0.0)
        return rw, ww, waw

    rw, ww, waw = lax.fori_loop(0, n, pass3, (zero, zero, zero), unroll=8)

    for copy in second:
        copy.wait_recv()
    wx[0] = wx[0] + recv_b[1]
    wx[n] = wx[n] + recv_b[0]
    high = send_b[2] + pltpu.roll(recv_b[2], m - 1, 1)
    strip3 = jnp.where(odd, pltpu.roll(recv_b[3], 1, 1), high)
    rest_of = jnp.logical_and(pair > 0, pair < n - 1)
    tw, ts = tb[5], tb[6] + jnp.where(odd, strip3, 0.0)
    te, tn = pltpu.roll(tw, m - 2, 1), jnp.where(odd, tb[7], strip3)
    faces = (tw, te, ts, tn, tb[8], tb[9])
    flux, _ = cell(*faces, tb[0], tb[1], tb[2], tb[3], None)
    waw = waw + jnp.where(rest_of, quadratic(faces, flux), 0.0)
    ts = jnp.where(jnp.logical_and(rest_of, odd), ts, 0.0)
    ww = ww + ts * ts
    rw = rw + ts * tb[12]
    for i in (0, n - 1):
        faces, flux, _ = row(i, image, strip3, False, False)
        w, _, s, _, b, t = faces
        rb, rt = vertical(i, rz_x)
        top = jnp.where(level == levels - 1, t, 0.0)
        rw = rw + (w * rx[i] + s * ry[i] + b * rb + top * rt)
        ww = ww + (w * w + s * s + b * b + top * top)
        waw = waw + quadratic(faces, flux)

    def finish(i, carry):
        faces, _, p = row(i, image, strip3, False, False)
        wy[i] = faces[2]
        p2[i] = p
        p0[i] = row(i, start, strip1, True, True)[2]
        rz[pl.ds(i, levels + 1, stride=n), :] = rz_x[i]
        wz[pl.ds(i, levels + 1, stride=n), :] = wz_x[i]
        return carry

    lane_row = lax.broadcasted_iota(jnp.int32, (1, m), 1)
    sums = jnp.zeros((1, m), F32)
    for k, part in enumerate((rr, rw, ww, waw)):
        whole = jnp.sum(jnp.sum(part, axis=0, keepdims=True), axis=1, keepdims=True)
        sums = jnp.where(lane_row == k, whole, sums)

    for k, (group, slot) in enumerate(zip(groups, slots)):
        row_b[k] = sums
        for j, device in enumerate(group):
            pltpu.make_async_remote_copy(
                src_ref=row_b.at[pl.ds(k, 1)],
                dst_ref=slot.at[pl.ds(j, 1)],
                send_sem=ar_send.at[k],
                recv_sem=ar_recv.at[k],
                device_id=device,
                device_id_type=MESH,
            ).start()
        if k == 0:
            lax.fori_loop(0, n, finish, 0, unroll=4)
        everything = pltpu.make_async_remote_copy(
            src_ref=slot, dst_ref=slot, send_sem=ar_send.at[k], recv_sem=ar_recv.at[k],
            device_id=group[0], device_id_type=MESH,
        )
        everything.wait_recv()
        sums = sums + jnp.sum(slot[...], axis=0)
        everything.wait_send()

    rr, rw, ww, waw = [
        jnp.sum(jnp.where(lane_row == k, sums, 0.0), axis=1, keepdims=True) for k in range(4)
    ]
    a0 = rr / rw
    grown = ww * a0 / rw
    b = grown - 1.0
    a1 = b * rr / (a0 * a0 * waw - grown * grown * rw)
    coef[0] = jnp.broadcast_to(a0 + a1 * grown, coef.shape[1:])
    coef[1] = jnp.broadcast_to(-a1 * a0, coef.shape[1:])
    for copy in first + second:
        copy.wait_send()


def combine_kernel(
    x_ref, y_ref, z_ref, rx, ry, rz, wx, wy, wz, p0, p1, p2, coef,
    ox_h, oy_h, oz_h, op_h, ox, oy, oz, op, sem,
):
    n = ox.shape[0]
    chunks = 5
    rows = n // chunks
    step = n
    c1, c2 = coef[0, 0:1, :], coef[1, 0:1, :]
    copies = []
    for k in range(chunks):

        def body(i, carry):
            ox[i] = x_ref[i] + (c1 * rx[i] + c2 * wx[i])
            oy[i] = y_ref[i] + (c1 * ry[i] + c2 * wy[i])
            op[i] = p0[i] + (c1 * p1[i] + c2 * p2[i])
            return carry

        lax.fori_loop(k * rows, (k + 1) * rows, body, 0)
        tall = oz.shape[0] // chunks

        def body_z(i, carry):
            at = pl.ds(pl.multiple_of(i * step, step), step)
            oz[at, :] = z_ref[at, :] + (c1 * rz[at, :] + c2 * wz[at, :])
            return carry

        lax.fori_loop(k * (tall // step), (k + 1) * (tall // step), body_z, 0)
        span = pl.ds(k * rows, rows)
        span_z = pl.ds(k * tall, tall)
        for j, (src, dst, at) in enumerate(
            ((ox, ox_h, span), (oy, oy_h, span), (oz, oz_h, span_z), (op, op_h, span))
        ):
            copy = pltpu.make_async_copy(src.at[at], dst.at[at], sem.at[k, j])
            copy.start()
            copies.append(copy)
    for copy in copies:
        copy.wait()


def local(px, py, metric, helmholtz, forcing, orientation, start_x, start_y, start_z):
    n, levels, m = helmholtz.shape
    face = (n, levels, m)
    longer = (n + 1, levels, m)
    taller = ((levels + 1) * n, m)
    start_z = jnp.transpose(start_z, (1, 0, 2)).reshape(taller)
    arguments = [
        pltpu.with_memory_space_constraint(a, pltpu.HBM)
        for a in (metric, helmholtz, forcing, orientation, start_x, start_y, start_z)
    ]
    shapes = [longer, face, taller, longer, face, taller, longer, face, taller, face, face, face, (2, 8, m)]
    held = pl.pallas_call(
        functools.partial(halo_kernel, px, py),
        out_shape=[pltpu.VMEM(shape, F32) for shape in shapes],
        in_specs=[pl.BlockSpec(memory_space=pl.ANY)] * 7,
        out_specs=[pl.BlockSpec(memory_space=pltpu.VMEM)] * len(shapes),
        scratch_shapes=[
            pltpu.VMEM((3,) + face, metric.dtype),
            pltpu.VMEM(face, helmholtz.dtype),
            pltpu.VMEM(face, forcing.dtype),
            pltpu.VMEM((n, m), jnp.int32),
            pltpu.VMEM(face, F32),
            pltpu.VMEM(face, F32),
            pltpu.VMEM(face, F32),
            pltpu.VMEM(face, F32),
            pltpu.VMEM((n, levels + 1, m), F32),
            pltpu.VMEM((n, levels + 1, m), F32),
            pltpu.VMEM((n, levels + 1, m), F32),
            pltpu.VMEM((16, levels, m), F32),
            pltpu.VMEM((3, levels, m), F32),
            pltpu.VMEM((4, levels, m), F32),
            pltpu.VMEM((2, 3, levels, m), F32),
            pltpu.VMEM((2, 3, levels, m), F32),
            pltpu.VMEM((2, levels, m), F32),
            pltpu.VMEM((2, levels, m), F32),
            pltpu.VMEM((2, 1, m), F32),
            pltpu.VMEM((3, 1, m), F32),
            pltpu.VMEM((len(PHASES), 1, m), F32),
        ]
        + [pltpu.VMEM((group_size(px, py, dims) - 1, 1, m), F32) for dims in PHASES]
        + [
            pltpu.SemaphoreType.DMA((7,)),
            pltpu.SemaphoreType.DMA((11,)),
            pltpu.SemaphoreType.DMA((11,)),
            pltpu.SemaphoreType.DMA((len(PHASES),)),
            pltpu.SemaphoreType.DMA((len(PHASES),)),
        ],
        compiler_params=pltpu.CompilerParams(
            collective_id=0, has_side_effects=True, vmem_limit_bytes=40 * 1024 * 1024
        ),
        name="halo",
    )(*arguments)
    outs = [face, face, taller, face]
    trace_x, trace_y, trace_z, pressure = pl.pallas_call(
        combine_kernel,
        out_shape=[jax.ShapeDtypeStruct(shape, F32) for shape in outs],
        in_specs=[pl.BlockSpec(memory_space=pltpu.VMEM)] * len(shapes),
        out_specs=[pl.BlockSpec(memory_space=pl.ANY)] * 4,
        scratch_shapes=[pltpu.VMEM(shape, F32) for shape in outs]
        + [pltpu.SemaphoreType.DMA((5, 4))],
        compiler_params=pltpu.CompilerParams(vmem_limit_bytes=20 * 1024 * 1024),
        name="combine",
    )(*held)
    trace_z = jnp.transpose(trace_z.reshape(levels + 1, n, m), (1, 0, 2))
    return trace_x, trace_y, trace_z, pressure


def solution(mesh):
    px, py = mesh.shape["px"], mesh.shape["py"]
    columns = P("px", None, "py")
    return jax.shard_map(
        functools.partial(local, px, py),
        mesh=mesh,
        in_specs=(P(None, "px", None, "py"), columns, columns, P("px", "py"), columns, columns, columns),
        out_specs=(columns,) * 4,
        check_vma=False,
    )
```
